32 devices in a mesh: by: 4 (over z), bx: 8 (over y, x, core).
Axes of the slice: x: 2, y: 2, z: 4, core: 2. Of those that a mesh axis runs over, the one named last changes fastest.
Arguments:
- wave_fn: float32 [1024, 2, 2, 1024], P('bx', None, None, 'by')
- left_env: float32 [1024, 5, 1024], P('bx')
- mpo_ten: float32 [5, 2, 2, 5], replicated
- right_env: float32 [1024, 5, 1024], P('by')
Outputs:
- output: float32 [1024, 2, 2, 1024], P('bx', None, None, 'by')
All inputs are finite; a program needn't handle non-finite values.
Results may differ from the reference program's by a relative error of at most 0.001.
Values sent between devices are 32-bit elements.
A program may use at most 1 GiB of HBM per device.

```python
import jax
import jax.numpy as jnp
from jax import lax

BOND_DIM = 1024
PHYS_DIM = 2
MPO_DIM = 5


def setup_inputs(seed: int = 0) -> dict:
    key = jax.random.key(seed)
    k_wave, k_left, k_mpo, k_right = jax.random.split(key, 4)
    wave_fn = jax.random.normal(k_wave, (BOND_DIM, PHYS_DIM, PHYS_DIM, BOND_DIM), jnp.float32)
    left_env = jax.random.normal(k_left, (BOND_DIM, MPO_DIM, BOND_DIM), jnp.float32) * (BOND_DIM ** -0.5)
    mpo_ten = jax.random.normal(k_mpo, (MPO_DIM, PHYS_DIM, PHYS_DIM, MPO_DIM), jnp.float32) * ((MPO_DIM * PHYS_DIM) ** -0.5)
    right_env = jax.random.normal(k_right, (BOND_DIM, MPO_DIM, BOND_DIM), jnp.float32) * ((MPO_DIM * BOND_DIM) ** -0.5)
    return {'wave_fn': wave_fn, 'left_env': left_env, 'mpo_ten': mpo_ten, 'right_env': right_env}


def reference(wave_fn, left_env, mpo_ten, right_env):
    row_block = min(BOND_DIM, 128)
    block_count = BOND_DIM // row_block
    left_blocks = left_env.reshape(block_count, row_block, MPO_DIM, BOND_DIM)

    def one_block(left_rows):
        stage_one = jnp.einsum('auc,cpqf->aupqf', left_rows.astype(jnp.float32), wave_fn.astype(jnp.float32))
        stage_two = jnp.einsum('aupqf,uspv->asvqf', stage_one, mpo_ten.astype(jnp.float32))
        stage_three = jnp.einsum('asvqf,vtqr->astrf', stage_two, mpo_ten.astype(jnp.float32))
        return jnp.einsum('astrf,brf->astb', stage_three, right_env.astype(jnp.float32))

    out_blocks = lax.map(one_block, left_blocks)
    return out_blocks.reshape(BOND_DIM, PHYS_DIM, PHYS_DIM, BOND_DIM)
```

```python
import functools

import jax
import jax.numpy as jnp
from jax import lax
from jax.experimental import pallas as pl
from jax.experimental.pallas import tpu as pltpu
from jax.sharding import PartitionSpec as P

MESH = pl.DeviceIdType.MESH
HIGHEST = lax.Precision.HIGHEST
NT = (((1,), (1,)), ((), ()))


def dot_nt(lhs, rhs):
    return lax.dot_general(lhs, rhs, NT, precision=HIGHEST, preferred_element_type=jnp.float32)


def kernel(x_ref, l_ref, w_ref, r_ref, y_ref, xg, rv, acc, vt, lg, pb, ra, rb, rx, ry, rp,
           x_up, x_dn, x_pt, x_in, l_out, l_pt, l_in, loc, s_sem, p_sem, r_sem):
    j, i = lax.axis_index('by'), lax.axis_index('bx')
    chip, core = lax.div(i, 2), lax.rem(i, 2)
    xb, yb = lax.rem(chip, 2), lax.div(chip, 2)
    xc, yc = chip + 1 - 2 * xb, chip + 2 - 4 * yb
    dc = xc + yc - chip
    partner = (j, i + 1 - 2 * core)
    rows = pl.ds(pl.multiple_of(core * 128, 128), 128)
    other_rows = pl.ds(pl.multiple_of((1 - core) * 128, 128), 128)

    def at(chip_, core_):
        return (j, 2 * chip_ + core_)

    def remote(src, dst, send, recv, device):
        return pltpu.make_async_remote_copy(src_ref=src, dst_ref=dst, send_sem=send, recv_sem=recv,
                                            device_id=device, device_id_type=MESH)

    def cols(chip_):
        return pl.ds(pl.multiple_of(chip_ * 256, 256), 256)

    load_r = pltpu.make_async_copy(r_ref.at[:, rows, :], rv, loc.at[0])
    load_x = pltpu.make_async_copy(x_ref, xg.at[j, :, rows, :], loc.at[1])
    load_l = pltpu.make_async_copy(l_ref.at[:, :, cols(chip)], lg.at[i], loc.at[2])
    load_x.start()
    load_r.start()
    load_l.start()

    barrier = pltpu.get_barrier_semaphore()
    near = [partner, at(xc, 0), at(xc, 1), at(yc, 0), at(yc, 1), at(dc, core)]
    for device in near:
        pl.semaphore_signal(barrier, inc=1, device_id=device, device_id_type=MESH)

    @pl.when(j > 0)
    def _():
        pl.semaphore_signal(barrier, inc=1, device_id=(j - 1, i), device_id_type=MESH)

    @pl.when(j < 3)
    def _():
        pl.semaphore_signal(barrier, inc=1, device_id=(j + 1, i), device_id_type=MESH)

    @pl.when((j > 0) & (j < 3))
    def _():
        pl.semaphore_wait(barrier, 8)

    @pl.when((j == 0) | (j == 3))
    def _():
        pl.semaphore_wait(barrier, 7)

    def x_copy(src, z, q, sems, device):
        return remote(src, xg.at[z, q, rows, :], sems.at[z, q], x_in.at[z, q, core], device)

    def x_held(z, q):
        return xg.at[z, q, rows, :]

    for q in range(4):
        @pl.when(j < 3)
        def _():
            x_copy(x_ref.at[q], j, q, x_up, (j + 1, i)).start()

        @pl.when(j > 0)
        def _():
            x_copy(x_ref.at[q], j, q, x_dn, (j - 1, i)).start()

        x_copy(x_ref.at[q], j, q, x_pt, partner).start()

    def l_copy(chip_, n):
        return remote(l_ref.at[:, :, cols(chip_)], lg.at[i], l_out.at[n], l_in.at[i], at(chip_, core))

    def l_pass(chip_, n):
        slot = 2 * chip_ + core
        return remote(lg.at[slot], lg.at[slot], l_pt.at[n], l_in.at[slot], partner)

    for n, chip_ in enumerate((xc, yc, dc)):
        l_copy(chip_, n).start()
    load_l.wait()
    l_pass(chip, 3).start()
    load_x.wait()
    load_r.wait()

    def arrive(z, q):
        x_copy(x_held(z, q), z, q, x_pt, partner).wait_recv()

    low = j < 2
    jm = jnp.where(low, j, 3 - j)

    def step(n, _):
        t, q = lax.div(n, 4), lax.rem(n, 4)

        @pl.when((t > 0) & (n < 16) & (j - t >= 0))
        def _():
            z = j - t
            arrive(z, q)

            @pl.when(j < 3)
            def _():
                x_copy(x_held(z, q), z, q, x_up, (j + 1, i)).start()

            x_copy(x_held(z, q), z, q, x_pt, partner).start()

        @pl.when((t > 0) & (n < 16) & (j + t <= 3))
        def _():
            z = j + t
            arrive(z, q)

            @pl.when(j > 0)
            def _():
                x_copy(x_held(z, q), z, q, x_dn, (j - 1, i)).start()

            x_copy(x_held(z, q), z, q, x_pt, partner).start()

        @pl.when(n == 12)
        def _():
            for m, chip_ in enumerate((xc, yc)):
                l_pass(chip_, m).wait_recv()
                l_pass(chip_, m).start()

        @pl.when(n == 15)
        def _():
            l_pass(dc, 2).wait_recv()
            l_pass(dc, 2).start()

        @pl.when(n > 0)
        def _():
            tt, qq = lax.div(n - 1, 4), lax.rem(n - 1, 4)
            zm = jnp.where(tt == 0, jm, jnp.where(tt == 1, 1 - jm, tt))
            z = jnp.where(low, zm, 3 - zm)
            remote(xg.at[z, qq, other_rows, :], xg.at[z, qq, other_rows, :], x_pt.at[z, qq],
                   x_in.at[z, qq, 1 - core], partner).wait_recv()
            lhs = rv[:, :, pl.ds(pl.multiple_of(z * 256, 256), 256)].reshape(640, 256)
            part = dot_nt(lhs, xg[z, qq]).reshape(5, 128, 256)
            dst = acc.at[:, :, pl.ds(pl.multiple_of(qq * 256, 256), 256)]

            @pl.when(tt == 0)
            def _():
                dst[...] = part

            @pl.when(tt > 0)
            def _():
                dst[...] += part

        return 0

    lax.fori_loop(0, 17, step, 0)

    def wt(u, s, p, v):
        return w_ref[((u * 2 + s) * 2 + p) * 5 + v]

    def sites(t):
        def tile(n, _):
            b = pl.ds(pl.multiple_of(n * 8, 8), 8)
            mid = []
            for p in range(2):
                parts = [acc[r, b, (p * 2 + q) * 256:(p * 2 + q + 1) * 256] for q in range(2) for r in range(5)]
                for v in range(5):
                    tot = None
                    for q in range(2):
                        for r in range(5):
                            term = parts[q * 5 + r] * wt(v, t, q, r)
                            tot = term if tot is None else tot + term
                    mid.append(tot)
            for u in range(5):
                for s in range(2):
                    tot = None
                    for p in range(2):
                        for v in range(5):
                            term = mid[p * 5 + v] * wt(u, s, p, v)
                            tot = term if tot is None else tot + term
                    vt[t, pl.ds(pl.multiple_of(s * 128 + n * 8, 8), 8), u * 256:(u + 1) * 256] = tot
            return 0

        lax.fori_loop(0, 16, tile, 0)

    def left(slots, t):
        lhs = jnp.concatenate(
            [jnp.concatenate([lg[slot, u] for u in range(5)], axis=1) for slot in slots], axis=0)
        return dot_nt(lhs, vt[t])

    def wait_left(chip_):
        slot = 2 * chip_ + 1 - core
        remote(lg.at[slot], lg.at[slot], l_pt.at[0], l_in.at[slot], partner).wait_recv()

    def send_far(h, t):
        if h == 0:
            return remote(pb.at[0, t], ra.at[t], s_sem.at[0, t], p_sem.at[0, t], at(xc, core))
        return remote(pb.at[1, t], rb.at[t], s_sem.at[1, t], p_sem.at[1, t], at(yc, core))

    def send_x(n, h, t):
        return remote(pb.at[n, t], rx.at[core, t], s_sem.at[n, t], r_sem.at[0, core, t], at(xc, h))

    def send_y(n, h, t):
        return remote(pb.at[n, t], ry.at[core, t], s_sem.at[n, t], r_sem.at[1, core, t], at(yc, h))

    def send_pt(t):
        return remote(pb.at[6, t], rp.at[t], s_sem.at[6, t], p_sem.at[2, t], partner)

    wait_left(dc)
    for t in range(2):
        sites(t)
        res = left((2 * dc, 2 * dc + 1), t)
        pb[0, t] = res[:128]
        pb[1, t] = res[128:]
        send_far(0, t).start()
        send_far(1, t).start()
    wait_left(xc)
    wait_left(yc)
    for t in range(2):
        res = left((2 * xc, 2 * yc + 1), t)
        pb[2, t] = res[:128]
        pb[3, t] = res[128:]
        send_x(2, 0, t).start()
        send_y(3, 1, t).start()
    for t in range(2):
        res = left((2 * yc, 2 * xc + 1), t)
        send_far(0, t).wait_recv()
        send_far(1, t).wait_recv()
        pb[4, t] = res[:128] + ra[t]
        pb[5, t] = res[128:] + rb[t]
        send_y(4, 0, t).start()
        send_x(5, 1, t).start()
    wait_left(chip)
    for t in range(2):
        res = left((2 * chip + 1 - core, 2 * chip + core), t)
        pb[6, t] = res[:128]
        pb[7, t] = res[128:]
        send_pt(t).start()
    for t in range(2):
        send_pt(t).wait_recv()
        for half in range(2):
            remote(rx.at[half, t], rx.at[half, t], s_sem.at[0, t], r_sem.at[0, half, t], partner).wait_recv()
            remote(ry.at[half, t], ry.at[half, t], s_sem.at[0, t], r_sem.at[1, half, t], partner).wait_recv()
        for s in range(2):
            lanes = slice(s * 128, (s + 1) * 128)
            y_ref[s * 2 + t, :, rows] = pb[7, t, :, lanes] + (rx[core, t, :, lanes] + ry[core, t, :, lanes])
            y_ref[s * 2 + t, :, other_rows] = rp[t, :, lanes] + (rx[1 - core, t, :, lanes] + ry[1 - core, t, :, lanes])

    def drain(n, _):
        z, q = lax.div(n, 4), lax.rem(n, 4)

        @pl.when((z <= j) & (j < 3))
        def _():
            x_copy(x_held(z, q), z, q, x_up, (j + 1, i)).wait_send()

        @pl.when((z >= j) & (j > 0))
        def _():
            x_copy(x_held(z, q), z, q, x_dn, (j - 1, i)).wait_send()

        x_copy(x_held(z, q), z, q, x_pt, partner).wait_send()
        return 0

    lax.fori_loop(0, 16, drain, 0)
    for n, chip_ in enumerate((xc, yc, dc)):
        l_copy(chip_, n).wait_send()
        l_pass(chip_, n).wait_send()
    l_pass(chip, 3).wait_send()
    for t in range(2):
        send_far(0, t).wait_send()
        send_far(1, t).wait_send()
        send_x(2, 0, t).wait_send()
        send_y(3, 1, t).wait_send()
        send_y(4, 0, t).wait_send()
        send_x(5, 1, t).wait_send()
        send_pt(t).wait_send()


def solution(mesh):
    def local_apply(wave, left, mpo, right):
        x = wave.reshape(128, 4, 256).transpose(1, 0, 2)
        f32, vmem, sem = jnp.float32, pltpu.VMEM, pltpu.SemaphoreType.DMA
        y = pl.pallas_call(
            kernel,
            out_shape=jax.ShapeDtypeStruct((4, 128, 256), f32),
            in_specs=[pl.BlockSpec(memory_space=pl.ANY), pl.BlockSpec(memory_space=pl.ANY),
                      pl.BlockSpec(memory_space=pltpu.SMEM), pl.BlockSpec(memory_space=pl.ANY)],
            out_specs=pl.BlockSpec(memory_space=pltpu.VMEM),
            scratch_shapes=[
                vmem((4, 4, 256, 256), f32), vmem((5, 128, 1024), f32), vmem((5, 128, 1024), f32),
                vmem((2, 256, 1280), f32), vmem((8, 5, 128, 256), f32), vmem((8, 2, 128, 256), f32),
                vmem((2, 128, 256), f32), vmem((2, 128, 256), f32), vmem((2, 2, 128, 256), f32),
                vmem((2, 2, 128, 256), f32), vmem((2, 128, 256), f32),
                sem((4, 4)), sem((4, 4)), sem((4, 4)), sem((4, 4, 2)), sem((3,)), sem((4,)), sem((8,)), sem((3,)),
                sem((7, 2)), sem((3, 2)), sem((2, 2, 2)),
            ],
            compiler_params=pltpu.CompilerParams(collective_id=0, has_side_effects=True,
                                                 vmem_limit_bytes=48 * 1024 * 1024),
        )(x, left.transpose(1, 0, 2), mpo.reshape(100), right.transpose(1, 0, 2))
        return y.reshape(2, 2, 128, 256).transpose(2, 0, 1, 3)

    return jax.shard_map(local_apply, mesh=mesh,
                         in_specs=(P('bx', None, None, 'by'), P('bx', None, None), P(), P('by', None, None)),
                         out_specs=P('bx', None, None, 'by'), check_vma=False)
```

```python
import functools

import jax
import jax.numpy as jnp
from jax import lax
from jax.experimental import pallas as pl
from jax.experimental.pallas import tpu as pltpu
from jax.sharding import PartitionSpec as P

MESH = pl.DeviceIdType.MESH
HIGHEST = lax.Precision.HIGHEST
NT = (((1,), (1,)), ((), ()))


def dot_nt(lhs, rhs):
    return lax.dot_general(lhs, rhs, NT, precision=HIGHEST, preferred_element_type=jnp.float32)


def kernel(x_ref, l_ref, w_hbm, r_ref, y_ref, xv, w_ref, xg, rv, acc, vt, lg, pb, ra, rb, rx, ry, rp,
           x_up, x_dn, x_pt, x_in, l_out, l_pt, l_in, loc, s_sem, p_sem, r_sem):
    j, i = lax.axis_index('by'), lax.axis_index('bx')
    chip, core = lax.div(i, 2), lax.rem(i, 2)
    xb, yb = lax.rem(chip, 2), lax.div(chip, 2)
    xc, yc = chip + 1 - 2 * xb, chip + 2 - 4 * yb
    dc = xc + yc - chip
    partner = (j, i + 1 - 2 * core)
    rows = pl.ds(pl.multiple_of(core * 128, 128), 128)
    other_rows = pl.ds(pl.multiple_of((1 - core) * 128, 128), 128)

    def at(chip_, core_):
        return (j, 2 * chip_ + core_)

    def remote(src, dst, send, recv, device):
        return pltpu.make_async_remote_copy(src_ref=src, dst_ref=dst, send_sem=send, recv_sem=recv,
                                            device_id=device, device_id_type=MESH)

    def cols(chip_):
        return pl.ds(pl.multiple_of(chip_ * 256, 256), 256)

    load_r = pltpu.make_async_copy(r_ref.at[:, rows, :], rv, loc.at[0])
    load_x = pltpu.make_async_copy(x_ref, xv, loc.at[1])
    load_w = pltpu.make_async_copy(w_hbm, w_ref, loc.at[3])
    load_l = pltpu.make_async_copy(l_ref.at[:, :, cols(chip)], lg.at[i], loc.at[2])
    load_x.start()
    load_w.start()
    load_r.start()
    load_l.start()

    barrier = pltpu.get_barrier_semaphore()
    near = [partner, at(xc, 0), at(xc, 1), at(yc, 0), at(yc, 1), at(dc, core)]
    for device in near:
        pl.semaphore_signal(barrier, inc=1, device_id=device, device_id_type=MESH)

    @pl.when(j > 0)
    def _():
        pl.semaphore_signal(barrier, inc=1, device_id=(j - 1, i), device_id_type=MESH)

    @pl.when(j < 3)
    def _():
        pl.semaphore_signal(barrier, inc=1, device_id=(j + 1, i), device_id_type=MESH)

    load_x.wait()
    for p in range(2):
        for half in range(2):
            for q in range(2):
                xg[j, p * 2 + q, rows, half * 128:(half + 1) * 128] = xv[pl.ds(p * 4 + half * 2 + q, 128, stride=8), :]

    @pl.when((j > 0) & (j < 3))
    def _():
        pl.semaphore_wait(barrier, 8)

    @pl.when((j == 0) | (j == 3))
    def _():
        pl.semaphore_wait(barrier, 7)

    def x_copy(src, z, q, sems, device):
        return remote(src, xg.at[z, q, rows, :], sems.at[z, q], x_in.at[z, q, core], device)

    def x_held(z, q):
        return xg.at[z, q, rows, :]

    for q in range(4):
        @pl.when(j < 3)
        def _():
            x_copy(x_held(j, q), j, q, x_up, (j + 1, i)).start()

        @pl.when(j > 0)
        def _():
            x_copy(x_held(j, q), j, q, x_dn, (j - 1, i)).start()

        x_copy(x_held(j, q), j, q, x_pt, partner).start()

    def l_copy(chip_, n):
        return remote(l_ref.at[:, :, cols(chip_)], lg.at[i], l_out.at[n], l_in.at[i], at(chip_, core))

    def l_pass(chip_, n):
        slot = 2 * chip_ + core
        return remote(lg.at[slot], lg.at[slot], l_pt.at[n], l_in.at[slot], partner)

    for n, chip_ in enumerate((xc, yc, dc)):
        l_copy(chip_, n).start()
    load_l.wait()
    l_pass(chip, 3).start()
    load_w.wait()
    load_r.wait()

    def arrive(z, q):
        x_copy(x_held(z, q), z, q, x_pt, partner).wait_recv()

    low = j < 2
    jm = jnp.where(low, j, 3 - j)

    def step(n, _):
        t, q = lax.div(n, 4), lax.rem(n, 4)

        @pl.when((t > 0) & (n < 16) & (j - t >= 0))
        def _():
            z = j - t
            arrive(z, q)

            @pl.when(j < 3)
            def _():
                x_copy(x_held(z, q), z, q, x_up, (j + 1, i)).start()

            x_copy(x_held(z, q), z, q, x_pt, partner).start()

        @pl.when((t > 0) & (n < 16) & (j + t <= 3))
        def _():
            z = j + t
            arrive(z, q)

            @pl.when(j > 0)
            def _():
                x_copy(x_held(z, q), z, q, x_dn, (j - 1, i)).start()

            x_copy(x_held(z, q), z, q, x_pt, partner).start()

        @pl.when(n == 12)
        def _():
            for m, chip_ in enumerate((xc, yc)):
                l_pass(chip_, m).wait_recv()
                l_pass(chip_, m).start()

        @pl.when(n == 15)
        def _():
            l_pass(dc, 2).wait_recv()
            l_pass(dc, 2).start()

        @pl.when(n > 0)
        def _():
            tt, qq = lax.div(n - 1, 4), lax.rem(n - 1, 4)
            zm = jnp.where(tt == 0, jm, jnp.where(tt == 1, 1 - jm, tt))
            z = jnp.where(low, zm, 3 - zm)
            remote(xg.at[z, qq, other_rows, :], xg.at[z, qq, other_rows, :], x_pt.at[z, qq],
                   x_in.at[z, qq, 1 - core], partner).wait_recv()
            lhs = rv[:, :, pl.ds(pl.multiple_of(z * 256, 256), 256)].reshape(640, 256)
            part = dot_nt(lhs, xg[z, qq]).reshape(5, 128, 256)
            dst = acc.at[:, :, pl.ds(pl.multiple_of(qq * 256, 256), 256)]

            @pl.when(tt == 0)
            def _():
                dst[...] = part

            @pl.when(tt > 0)
            def _():
                dst[...] += part

        return 0

    lax.fori_loop(0, 17, step, 0)

    def wt(u, s, p, v):
        return w_ref[u, s, p, v]

    def sites(t):
        def tile(n, _):
            b = pl.ds(pl.multiple_of(n * 8, 8), 8)
            mid = []
            for p in range(2):
                parts = [acc[r, b, (p * 2 + q) * 256:(p * 2 + q + 1) * 256] for q in range(2) for r in range(5)]
                for v in range(5):
                    tot = None
                    for q in range(2):
                        for r in range(5):
                            term = parts[q * 5 + r] * wt(v, t, q, r)
                            tot = term if tot is None else tot + term
                    mid.append(tot)
            for u in range(5):
                for s in range(2):
                    tot = None
                    for p in range(2):
                        for v in range(5):
                            term = mid[p * 5 + v] * wt(u, s, p, v)
                            tot = term if tot is None else tot + term
                    vt[t, pl.ds(pl.multiple_of(s * 128 + n * 8, 8), 8), u * 256:(u + 1) * 256] = tot
            return 0

        lax.fori_loop(0, 16, tile, 0)

    def left(slots, t):
        lhs = jnp.concatenate(
            [jnp.concatenate([lg[slot, u] for u in range(5)], axis=1) for slot in slots], axis=0)
        return dot_nt(lhs, vt[t])

    def wait_left(chip_):
        slot = 2 * chip_ + 1 - core
        remote(lg.at[slot], lg.at[slot], l_pt.at[0], l_in.at[slot], partner).wait_recv()

    def send_far(h, t):
        if h == 0:
            return remote(pb.at[0, t], ra.at[t], s_sem.at[0, t], p_sem.at[0, t], at(xc, core))
        return remote(pb.at[1, t], rb.at[t], s_sem.at[1, t], p_sem.at[1, t], at(yc, core))

    def send_x(n, h, t):
        return remote(pb.at[n, t], rx.at[core, t], s_sem.at[n, t], r_sem.at[0, core, t], at(xc, h))

    def send_y(n, h, t):
        return remote(pb.at[n, t], ry.at[core, t], s_sem.at[n, t], r_sem.at[1, core, t], at(yc, h))

    def send_pt(t):
        return remote(pb.at[6, t], rp.at[t], s_sem.at[6, t], p_sem.at[2, t], partner)

    wait_left(dc)
    for t in range(2):
        sites(t)
        res = left((2 * dc, 2 * dc + 1), t)
        pb[0, t] = res[:128]
        pb[1, t] = res[128:]
        send_far(0, t).start()
        send_far(1, t).start()
    wait_left(xc)
    wait_left(yc)
    for t in range(2):
        res = left((2 * xc, 2 * yc + 1), t)
        pb[2, t] = res[:128]
        pb[3, t] = res[128:]
        send_x(2, 0, t).start()
        send_y(3, 1, t).start()
    for t in range(2):
        res = left((2 * yc, 2 * xc + 1), t)
        send_far(0, t).wait_recv()
        send_far(1, t).wait_recv()
        pb[4, t] = res[:128] + ra[t]
        pb[5, t] = res[128:] + rb[t]
        send_y(4, 0, t).start()
        send_x(5, 1, t).start()
    wait_left(chip)
    for t in range(2):
        res = left((2 * chip + 1 - core, 2 * chip + core), t)
        pb[6, t] = res[:128]
        pb[7, t] = res[128:]
        send_pt(t).start()
    for t in range(2):
        send_pt(t).wait_recv()
        for half in range(2):
            remote(rx.at[half, t], rx.at[half, t], s_sem.at[0, t], r_sem.at[0, half, t], partner).wait_recv()
            remote(ry.at[half, t], ry.at[half, t], s_sem.at[0, t], r_sem.at[1, half, t], partner).wait_recv()
        for s in range(2):
            lanes = slice(s * 128, (s + 1) * 128)
            y_ref[pl.ds(s * 4 + core * 2 + t, 128, stride=8), :] = (
                pb[7, t, :, lanes] + (rx[core, t, :, lanes] + ry[core, t, :, lanes]))
            y_ref[pl.ds(s * 4 + (1 - core) * 2 + t, 128, stride=8), :] = (
                rp[t, :, lanes] + (rx[1 - core, t, :, lanes] + ry[1 - core, t, :, lanes]))

    def drain(n, _):
        z, q = lax.div(n, 4), lax.rem(n, 4)

        @pl.when((z <= j) & (j < 3))
        def _():
            x_copy(x_held(z, q), z, q, x_up, (j + 1, i)).wait_send()

        @pl.when((z >= j) & (j > 0))
        def _():
            x_copy(x_held(z, q), z, q, x_dn, (j - 1, i)).wait_send()

        x_copy(x_held(z, q), z, q, x_pt, partner).wait_send()
        return 0

    lax.fori_loop(0, 16, drain, 0)
    for n, chip_ in enumerate((xc, yc, dc)):
        l_copy(chip_, n).wait_send()
        l_pass(chip_, n).wait_send()
    l_pass(chip, 3).wait_send()
    for t in range(2):
        send_far(0, t).wait_send()
        send_far(1, t).wait_send()
        send_x(2, 0, t).wait_send()
        send_y(3, 1, t).wait_send()
        send_y(4, 0, t).wait_send()
        send_x(5, 1, t).wait_send()
        send_pt(t).wait_send()


def solution(mesh):
    def local_apply(wave, left, mpo, right):
        x = wave.reshape(128, 2, 2, 2, 128).transpose(0, 1, 3, 2, 4).reshape(1024, 128)
        f32, vmem, sem = jnp.float32, pltpu.VMEM, pltpu.SemaphoreType.DMA
        y = pl.pallas_call(
            kernel,
            out_shape=jax.ShapeDtypeStruct((1024, 128), f32),
            in_specs=[pl.BlockSpec(memory_space=pltpu.HBM), pl.BlockSpec(memory_space=pltpu.HBM),
                      pl.BlockSpec(memory_space=pltpu.HBM), pl.BlockSpec(memory_space=pltpu.HBM)],
            out_specs=pl.BlockSpec(memory_space=pltpu.VMEM),
            scratch_shapes=[
                vmem((1024, 128), f32), pltpu.SMEM((5, 2, 2, 5), f32),
                vmem((4, 4, 256, 256), f32), vmem((5, 128, 1024), f32), vmem((5, 128, 1024), f32),
                vmem((2, 256, 1280), f32), vmem((8, 5, 128, 256), f32), vmem((8, 2, 128, 256), f32),
                vmem((2, 128, 256), f32), vmem((2, 128, 256), f32), vmem((2, 2, 128, 256), f32),
                vmem((2, 2, 128, 256), f32), vmem((2, 128, 256), f32),
                sem((4, 4)), sem((4, 4)), sem((4, 4)), sem((4, 4, 2)), sem((3,)), sem((4,)), sem((8,)), sem((4,)),
                sem((7, 2)), sem((3, 2)), sem((2, 2, 2)),
            ],
            compiler_params=pltpu.CompilerParams(collective_id=0, has_side_effects=True,
                                                 vmem_limit_bytes=53 * 1024 * 1024),
        )(x, left.transpose(1, 0, 2), mpo, right.transpose(1, 0, 2))
        return y.reshape(128, 2, 2, 2, 128).transpose(0, 1, 3, 2, 4).reshape(128, 2, 2, 256)

    return jax.shard_map(local_apply, mesh=mesh,
                         in_specs=(P('bx', None, None, 'by'), P('bx', None, None), P(), P('by', None, None)),
                         out_specs=P('bx', None, None, 'by'), check_vma=False)
```

```python
import functools

import jax
import jax.numpy as jnp
from jax import lax
from jax.experimental import pallas as pl
from jax.experimental.pallas import tpu as pltpu
from jax.sharding import PartitionSpec as P

MESH = pl.DeviceIdType.MESH
HIGHEST = lax.Precision.HIGHEST
NT = (((1,), (1,)), ((), ()))


def dot_nt(lhs, rhs):
    return lax.dot_general(lhs, rhs, NT, precision=HIGHEST, preferred_element_type=jnp.float32)


def kernel(x_ref, l_ref, w_hbm, r_ref, y_ref, xv, w_ref, xg, rv, acc, zp, vt, lg, pb, ra, rb, rx, ry, rp,
           x_up, x_dn, x_pt, x_in, l_out, l_pt, l_in, loc, s_sem, p_sem, r_sem, rq, q_out, q_in):
    j, i = lax.axis_index('by'), lax.axis_index('bx')
    chip, core = lax.div(i, 2), lax.rem(i, 2)
    xb, yb = lax.rem(chip, 2), lax.div(chip, 2)
    xc, yc = chip + 1 - 2 * xb, chip + 2 - 4 * yb
    dc = xc + yc - chip
    partner = (j, i + 1 - 2 * core)
    rows = pl.ds(pl.multiple_of(core * 128, 128), 128)
    other_rows = pl.ds(pl.multiple_of((1 - core) * 128, 128), 128)

    def at(chip_, core_):
        return (j, 2 * chip_ + core_)

    def remote(src, dst, send, recv, device):
        return pltpu.make_async_remote_copy(src_ref=src, dst_ref=dst, send_sem=send, recv_sem=recv,
                                            device_id=device, device_id_type=MESH)

    def cols(chip_):
        return pl.ds(pl.multiple_of(chip_ * 256, 256), 256)

    load_r = pltpu.make_async_copy(r_ref.at[:, rows, :], rv, loc.at[0])
    load_x = pltpu.make_async_copy(x_ref, xv, loc.at[1])
    load_w = pltpu.make_async_copy(w_hbm, w_ref, loc.at[3])
    load_l = pltpu.make_async_copy(l_ref.at[:, :, cols(chip)], lg.at[i], loc.at[2])
    load_x.start()
    load_w.start()
    load_r.start()
    load_l.start()

    barrier = pltpu.get_barrier_semaphore()
    end = (j == 0) | (j == 3)
    pair = j + 1 - 2 * lax.rem(j, 2)
    near = [partner, at(xc, 0), at(xc, 1), at(yc, 0), at(yc, 1), at(dc, core),
            (pair, 2 * xc + core), (pair, 2 * yc + core), (pair, 2 * chip + 1 - core)]
    for device in near:
        pl.semaphore_signal(barrier, inc=1, device_id=device, device_id_type=MESH)

    @pl.when(j > 0)
    def _():
        pl.semaphore_signal(barrier, inc=1, device_id=(j - 1, i), device_id_type=MESH)

    @pl.when(j < 3)
    def _():
        pl.semaphore_signal(barrier, inc=1, device_id=(j + 1, i), device_id_type=MESH)

    load_x.wait()
    for p in range(2):
        for half in range(2):
            for q in range(2):
                xg[j, p * 2 + q, rows, half * 128:(half + 1) * 128] = xv[pl.ds(p * 4 + half * 2 + q, 128, stride=8), :]

    @pl.when((j > 0) & (j < 3))
    def _():
        pl.semaphore_wait(barrier, 11)

    @pl.when((j == 0) | (j == 3))
    def _():
        pl.semaphore_wait(barrier, 10)

    def x_copy(src, z, q, sems, device):
        return remote(src, xg.at[z, q, rows, :], sems.at[z, q], x_in.at[z, q, core], device)

    def x_held(z, q):
        return xg.at[z, q, rows, :]

    for q in range(4):
        @pl.when(j < 3)
        def _():
            x_copy(x_held(j, q), j, q, x_up, (j + 1, i)).start()

        @pl.when(j > 0)
        def _():
            x_copy(x_held(j, q), j, q, x_dn, (j - 1, i)).start()

        x_copy(x_held(j, q), j, q, x_pt, partner).start()

    def l_copy(chip_, n):
        return remote(l_ref.at[:, :, cols(chip_)], lg.at[i], l_out.at[n], l_in.at[i], at(chip_, core))

    def l_pass(chip_, n):
        slot = 2 * chip_ + core
        return remote(lg.at[slot], lg.at[slot], l_pt.at[n], l_in.at[slot], partner)

    for n, chip_ in enumerate((xc, yc, dc)):
        l_copy(chip_, n).start()
    load_l.wait()
    l_pass(chip, 3).start()
    load_w.wait()
    load_r.wait()

    def arrive(z, q):
        x_copy(x_held(z, q), z, q, x_pt, partner).wait_recv()

    def wt(u, s, p, v):
        return w_ref[u, s, p, v]

    def field(r, p, q, b):
        return acc[r, b, (p * 2 + q) * 256:(p * 2 + q + 1) * 256]

    def dots(terms):
        total = None
        for weight, value in terms:
            total = value * weight if total is None else total + value * weight
        return total

    def tiles(body):
        def tile(n, _):
            body(pl.ds(pl.multiple_of(n * 8, 8), 8), n * 8)
            return 0

        lax.fori_loop(0, 16, tile, 0)

    def sites_first(b, start):
        parts = [(q, r, field(r, 0, q, b)) for q in range(2) for r in range(5)]
        for t in range(2):
            mid = [dots((wt(v, t, q, r), x) for q, r, x in parts) for v in range(5)]
            for s in range(2):
                into = pl.ds(pl.multiple_of(s * 128 + start, 8), 8)
                for u in range(5):
                    vt[t, into, u * 256:(u + 1) * 256] = dots((wt(u, s, 0, v), mid[v]) for v in range(5))

    def sites_second(b, start):
        parts = [field(r, 1, 0, b) for r in range(5)]
        for t in range(2):
            for v in range(5):
                zp[t, v, b, :] = dots((wt(v, t, 0, r), parts[r]) for r in range(5))

    def sites_last(t):
        def body(b, start):
            parts = [field(r, 1, 1, b) for r in range(5)]
            mid = [zp[t, v, b, :] + dots((wt(v, t, 1, r), parts[r]) for r in range(5)) for v in range(5)]
            for s in range(2):
                into = pl.ds(pl.multiple_of(s * 128 + start, 8), 8)
                for u in range(5):
                    vt[t, into, u * 256:(u + 1) * 256] += dots((wt(u, s, 1, v), mid[v]) for v in range(5))

        tiles(body)

    low = j < 2
    jm = jnp.where(low, j, 3 - j)

    def step(n, _):
        t, q = lax.div(n, 4), lax.rem(n, 4)

        @pl.when((t > 0) & (n < 16) & (j - t >= 0))
        def _():
            z = j - t
            arrive(z, q)

            @pl.when(j < 3)
            def _():
                x_copy(x_held(z, q), z, q, x_up, (j + 1, i)).start()

            x_copy(x_held(z, q), z, q, x_pt, partner).start()

        @pl.when((t > 0) & (n < 16) & (j + t <= 3))
        def _():
            z = j + t
            arrive(z, q)

            @pl.when(j > 0)
            def _():
                x_copy(x_held(z, q), z, q, x_dn, (j - 1, i)).start()

            x_copy(x_held(z, q), z, q, x_pt, partner).start()

        @pl.when(n == 12)
        def _():
            for m, chip_ in enumerate((xc, yc)):
                l_pass(chip_, m).wait_recv()
                l_pass(chip_, m).start()

        @pl.when(n == 15)
        def _():
            l_pass(dc, 2).wait_recv()
            l_pass(dc, 2).start()

        @pl.when(n > 0)
        def _():
            tt, qq = lax.div(n - 1, 4), lax.rem(n - 1, 4)
            zm = jnp.where(tt == 0, jm, jnp.where(tt == 1, 1 - jm, tt))
            z = jnp.where(low, zm, 3 - zm)
            remote(xg.at[z, qq, other_rows, :], xg.at[z, qq, other_rows, :], x_pt.at[z, qq],
                   x_in.at[z, qq, 1 - core], partner).wait_recv()
            lhs = rv[:, :, pl.ds(pl.multiple_of(z * 256, 256), 256)].reshape(640, 256)
            part = dot_nt(lhs, xg[z, qq]).reshape(5, 128, 256)
            dst = acc.at[:, :, pl.ds(pl.multiple_of(qq * 256, 256), 256)]

            @pl.when(tt == 0)
            def _():
                dst[...] = part

            @pl.when(tt > 0)
            def _():
                dst[...] += part

        @pl.when(n == 14)
        def _():
            tiles(sites_first)

        @pl.when(n == 15)
        def _():
            tiles(sites_second)

        return 0

    lax.fori_loop(0, 17, step, 0)

    def left(first, second, t):
        lhs = jnp.concatenate(
            [jnp.concatenate([lg[slot, u] for u in range(5)], axis=1) for slot in (first, second)], axis=0)
        return dot_nt(lhs, vt[t])

    def wait_left(chip_):
        slot = 2 * chip_ + 1 - core
        remote(lg.at[slot], lg.at[slot], l_pt.at[0], l_in.at[slot], partner).wait_recv()

    def send_far(h, t):
        if h == 0:
            return remote(pb.at[0, t], ra.at[t], s_sem.at[0, t], p_sem.at[0, t], at(xc, core))
        return remote(pb.at[1, t], rb.at[t], s_sem.at[1, t], p_sem.at[1, t], at(yc, core))

    def send_x(n, h, t):
        return remote(pb.at[n, t], rx.at[core, t], s_sem.at[n, t], r_sem.at[0, core, t], at(xc, h))

    def send_y(n, h, t):
        return remote(pb.at[n, t], ry.at[core, t], s_sem.at[n, t], r_sem.at[1, core, t], at(yc, h))

    def send_pt(t):
        return remote(pb.at[6, t], rp.at[t], s_sem.at[6, t], p_sem.at[2, t], partner)

    def send_via(h):
        return remote(pb.at[2 + h, 0], rq.at[h], s_sem.at[2 + h, 0], q_in.at[h], (pair, 2 * (yc if h else xc) + core))

    def send_back(h):
        land = ry if h else rx
        return remote(rq.at[h], land.at[core, 0], q_out.at[h], r_sem.at[h, core, 0], (pair, 2 * chip + h))

    wait_left(dc)
    wait_left(xc)
    wait_left(yc)
    wait_left(chip)

    def stage(n, _):
        role = jnp.where(n < 4, lax.rem(n, 2), jnp.where((n == 4) | (n == 7), 3, 2))
        t = jnp.where(n < 4, lax.div(n, 2), lax.div(n - 4, 2))

        @pl.when((n == 0) | (n == 2))
        def _():
            sites_last(t)

        def pick(far, near, via, own):
            return jnp.where(role == 0, far, jnp.where(role == 1, near, jnp.where(role == 2, via, own)))

        first = pick(2 * dc, 2 * xc, 2 * yc, 2 * chip + 1 - core)
        second = pick(2 * dc + 1, 2 * yc + 1, 2 * xc + 1, 2 * chip + core)
        res = left(first, second, t)

        @pl.when(role != 2)
        def _():
            pb[2 * role, t] = res[:128]
            pb[2 * role + 1, t] = res[128:]

        @pl.when((n == 6) & jnp.logical_not(end))
        def _():
            for h in range(2):
                send_via(h).wait_recv()
                send_back(h).start()

        @pl.when(role == 2)
        def _():
            send_far(0, t).wait_recv()
            send_far(1, t).wait_recv()
            pb[4, t] = res[:128] + ra[t]
            pb[5, t] = res[128:] + rb[t]
            send_y(4, 0, t).start()
            send_x(5, 1, t).start()

        @pl.when(role == 0)
        def _():
            send_far(0, t).start()
            send_far(1, t).start()

        @pl.when((role == 1) & (end & (t == 0)))
        def _():
            send_via(0).start()
            send_via(1).start()

        @pl.when((role == 1) & jnp.logical_not(end & (t == 0)))
        def _():
            send_x(2, 0, t).start()
            send_y(3, 1, t).start()

        @pl.when(role == 3)
        def _():
            send_pt(t).start()

        return 0

    lax.fori_loop(0, 8, stage, 0)

    def drain(n, _):
        z, q = lax.div(n, 4), lax.rem(n, 4)

        @pl.when((z <= j) & (j < 3))
        def _():
            x_copy(x_held(z, q), z, q, x_up, (j + 1, i)).wait_send()

        @pl.when((z >= j) & (j > 0))
        def _():
            x_copy(x_held(z, q), z, q, x_dn, (j - 1, i)).wait_send()

        x_copy(x_held(z, q), z, q, x_pt, partner).wait_send()
        return 0

    lax.fori_loop(0, 16, drain, 0)
    for n, chip_ in enumerate((xc, yc, dc)):
        l_copy(chip_, n).wait_send()
        l_pass(chip_, n).wait_send()
    l_pass(chip, 3).wait_send()
    for t in range(2):
        send_pt(t).wait_recv()
        for half in range(2):
            remote(rx.at[half, t], rx.at[half, t], s_sem.at[0, t], r_sem.at[0, half, t], partner).wait_recv()
            remote(ry.at[half, t], ry.at[half, t], s_sem.at[0, t], r_sem.at[1, half, t], partner).wait_recv()
        for s in range(2):
            lanes = slice(s * 128, (s + 1) * 128)
            y_ref[pl.ds(s * 4 + core * 2 + t, 128, stride=8), :] = (
                pb[7, t, :, lanes] + (rx[core, t, :, lanes] + ry[core, t, :, lanes]))
            y_ref[pl.ds(s * 4 + (1 - core) * 2 + t, 128, stride=8), :] = (
                rp[t, :, lanes] + (rx[1 - core, t, :, lanes] + ry[1 - core, t, :, lanes]))

    @pl.when(jnp.logical_not(end))
    def _():
        for h in range(2):
            send_back(h).wait_send()

    for t in range(2):
        send_far(0, t).wait_send()
        send_far(1, t).wait_send()
        send_x(2, 0, t).wait_send()
        send_y(3, 1, t).wait_send()
        send_y(4, 0, t).wait_send()
        send_x(5, 1, t).wait_send()
        send_pt(t).wait_send()


def solution(mesh):
    def local_apply(wave, left, mpo, right):
        x = wave.reshape(128, 2, 2, 2, 128).transpose(0, 1, 3, 2, 4).reshape(1024, 128)
        f32, vmem, sem = jnp.float32, pltpu.VMEM, pltpu.SemaphoreType.DMA
        y = pl.pallas_call(
            kernel,
            out_shape=jax.ShapeDtypeStruct((1024, 128), f32),
            in_specs=[pl.BlockSpec(memory_space=pltpu.HBM), pl.BlockSpec(memory_space=pltpu.HBM),
                      pl.BlockSpec(memory_space=pltpu.HBM), pl.BlockSpec(memory_space=pltpu.HBM)],
            out_specs=pl.BlockSpec(memory_space=pltpu.VMEM),
            scratch_shapes=[
                vmem((1024, 128), f32), pltpu.SMEM((5, 2, 2, 5), f32),
                vmem((4, 4, 256, 256), f32), vmem((5, 128, 1024), f32), vmem((5, 128, 1024), f32),
                vmem((2, 5, 128, 256), f32),
                vmem((2, 256, 1280), f32), vmem((8, 5, 128, 256), f32), vmem((8, 2, 128, 256), f32),
                vmem((2, 128, 256), f32), vmem((2, 128, 256), f32), vmem((2, 2, 128, 256), f32),
                vmem((2, 2, 128, 256), f32), vmem((2, 128, 256), f32),
                sem((4, 4)), sem((4, 4)), sem((4, 4)), sem((4, 4, 2)), sem((3,)), sem((4,)), sem((8,)), sem((4,)),
                sem((7, 2)), sem((3, 2)), sem((2, 2, 2)),
                vmem((2, 128, 256), f32), sem((2,)), sem((2,)),
            ],
            compiler_params=pltpu.CompilerParams(collective_id=0, has_side_effects=True,
                                                 vmem_limit_bytes=53 * 1024 * 1024),
        )(x, left.transpose(1, 0, 2), mpo, right.transpose(1, 0, 2))
        return y.reshape(128, 2, 2, 2, 128).transpose(0, 1, 3, 2, 4).reshape(128, 2, 2, 256)

    return jax.shard_map(local_apply, mesh=mesh,
                         in_specs=(P('bx', None, None, 'by'), P('bx', None, None), P(), P('by', None, None)),
                         out_specs=P('bx', None, None, 'by'), check_vma=False)
```

```python
import functools

import jax
import jax.numpy as jnp
from jax import lax
from jax.experimental import pallas as pl
from jax.experimental.pallas import tpu as pltpu
from jax.sharding import PartitionSpec as P

MESH = pl.DeviceIdType.MESH
HIGHEST = lax.Precision.HIGHEST
NT = (((1,), (1,)), ((), ()))


def dot_nt(lhs, rhs):
    return lax.dot_general(lhs, rhs, NT, precision=HIGHEST, preferred_element_type=jnp.float32)


def kernel(x_ref, l_ref, w_hbm, r_ref, y_ref, xv, w_ref, xg, rv, acc, zp, vt, lg, pb, ra, rb, rx, ry, rp,
           x_up, x_dn, x_pt, x_in, l_out, l_pt, l_in, loc, s_sem, p_sem, r_sem, rq, q_out, q_in):
    j, i = lax.axis_index('by'), lax.axis_index('bx')
    chip, core = lax.div(i, 2), lax.rem(i, 2)
    xb, yb = lax.rem(chip, 2), lax.div(chip, 2)
    xc, yc = chip + 1 - 2 * xb, chip + 2 - 4 * yb
    dc = xc + yc - chip
    partner = (j, i + 1 - 2 * core)
    rows = pl.ds(pl.multiple_of(core * 128, 128), 128)
    other_rows = pl.ds(pl.multiple_of((1 - core) * 128, 128), 128)

    def at(chip_, core_):
        return (j, 2 * chip_ + core_)

    def remote(src, dst, send, recv, device):
        return pltpu.make_async_remote_copy(src_ref=src, dst_ref=dst, send_sem=send, recv_sem=recv,
                                            device_id=device, device_id_type=MESH)

    def cols(chip_):
        return pl.ds(pl.multiple_of(chip_ * 256, 256), 256)

    load_r = pltpu.make_async_copy(r_ref.at[:, rows, :], rv, loc.at[0])
    load_x = pltpu.make_async_copy(x_ref, xv, loc.at[1])
    load_w = pltpu.make_async_copy(w_hbm, w_ref, loc.at[3])
    load_l = pltpu.make_async_copy(l_ref.at[:, :, cols(chip)], lg.at[i], loc.at[2])
    load_x.start()
    load_w.start()
    load_r.start()
    load_l.start()

    barrier = pltpu.get_barrier_semaphore()
    end = (j == 0) | (j == 3)
    pair = j + 1 - 2 * lax.rem(j, 2)
    near = [partner, at(xc, 0), at(xc, 1), at(yc, 0), at(yc, 1), at(dc, core),
            (pair, 2 * xc + core), (pair, 2 * yc + core), (pair, 2 * chip + 1 - core)]
    for device in near:
        pl.semaphore_signal(barrier, inc=1, device_id=device, device_id_type=MESH)

    @pl.when(j > 0)
    def _():
        pl.semaphore_signal(barrier, inc=1, device_id=(j - 1, i), device_id_type=MESH)

    @pl.when(j < 3)
    def _():
        pl.semaphore_signal(barrier, inc=1, device_id=(j + 1, i), device_id_type=MESH)

    load_x.wait()
    for p in range(2):
        for half in range(2):
            for q in range(2):
                xg[j, p * 2 + q, rows, half * 128:(half + 1) * 128] = xv[pl.ds(p * 4 + half * 2 + q, 128, stride=8), :]

    @pl.when((j > 0) & (j < 3))
    def _():
        pl.semaphore_wait(barrier, 11)

    @pl.when((j == 0) | (j == 3))
    def _():
        pl.semaphore_wait(barrier, 10)

    def x_copy(src, z, q, sems, device):
        return remote(src, xg.at[z, q, rows, :], sems.at[z, q], x_in.at[z, q, core], device)

    def x_held(z, q):
        return xg.at[z, q, rows, :]

    for q in range(4):
        @pl.when(j < 3)
        def _():
            x_copy(x_held(j, q), j, q, x_up, (j + 1, i)).start()

        @pl.when(j > 0)
        def _():
            x_copy(x_held(j, q), j, q, x_dn, (j - 1, i)).start()

        x_copy(x_held(j, q), j, q, x_pt, partner).start()

    def l_copy(chip_, n):
        return remote(l_ref.at[:, :, cols(chip_)], lg.at[i], l_out.at[n], l_in.at[i], at(chip_, core))

    def l_pass(chip_, n):
        slot = 2 * chip_ + core
        return remote(lg.at[slot], lg.at[slot], l_pt.at[n], l_in.at[slot], partner)

    for n, chip_ in enumerate((xc, yc, dc)):
        l_copy(chip_, n).start()
    load_l.wait()
    l_pass(chip, 3).start()
    load_w.wait()
    load_r.wait()

    def arrive(z, q):
        x_copy(x_held(z, q), z, q, x_pt, partner).wait_recv()

    def wt(u, s, p, v):
        return w_ref[u, s, p, v]

    def field(r, p, q, b):
        return acc[r, b, (p * 2 + q) * 256:(p * 2 + q + 1) * 256]

    def dots(terms):
        total = None
        for weight, value in terms:
            total = value * weight if total is None else total + value * weight
        return total

    def tiles(body):
        def tile(n, _):
            body(pl.ds(pl.multiple_of(n * 16, 16), 16), n * 16)
            return 0

        lax.fori_loop(0, 8, tile, 0)

    def sites_first(t):
        def body(b, start):
            parts = [(q, r, field(r, 0, q, b)) for q in range(2) for r in range(5)]
            mid = [dots((wt(v, t, q, r), x) for q, r, x in parts) for v in range(5)]
            for s in range(2):
                into = pl.ds(pl.multiple_of(s * 128 + start, 16), 16)
                for u in range(5):
                    vt[t, into, u * 256:(u + 1) * 256] = dots((wt(u, s, 0, v), mid[v]) for v in range(5))

        tiles(body)

    def sites_second(b, start):
        parts = [field(r, 1, 0, b) for r in range(5)]
        for t in range(2):
            for v in range(5):
                zp[t, v, b, :] = dots((wt(v, t, 0, r), parts[r]) for r in range(5))

    def sites_last(t, half):
        def tile(n, _):
            b = pl.ds(pl.multiple_of(n * 32, 32), 32)

            def lanes(first):
                return pl.ds(pl.multiple_of(first + half * 128, 128), 128)

            parts = [acc[r, b, lanes(768)] for r in range(5)]
            mid = [zp[t, v, b, lanes(0)] + dots((wt(v, t, 1, r), parts[r]) for r in range(5)) for v in range(5)]
            for s in range(2):
                into = pl.ds(pl.multiple_of(s * 128 + n * 32, 32), 32)
                for u in range(5):
                    vt[t, into, lanes(u * 256)] += dots((wt(u, s, 1, v), mid[v]) for v in range(5))
            return 0

        lax.fori_loop(0, 4, tile, 0)

    low = j < 2
    jm = jnp.where(low, j, 3 - j)

    def pass_rest():
        for n, chip_ in ((2, dc), (1, yc)):
            l_pass(chip_, n).wait_recv()
            l_pass(chip_, n).start()

    def wait_partner(z, q):
        held = xg.at[z, q, other_rows, :]
        remote(held, held, x_pt.at[z, q], x_in.at[z, q, 1 - core], partner).wait_recv()

    def right_part(z):
        return rv[:, :, pl.ds(pl.multiple_of(z * 256, 256), 256)].reshape(640, 256)

    def multiply(m, _):
        t, q = lax.div(m, 4), lax.rem(m, 4)
        zm = jnp.where(t == 0, jm, jnp.where(t == 1, 1 - jm, t))
        z = jnp.where(low, zm, 3 - zm)
        wait_partner(z, q)
        part = dot_nt(right_part(z), xg[z, q]).reshape(5, 128, 256)
        dst = acc.at[:, :, pl.ds(pl.multiple_of(q * 256, 256), 256)]

        @pl.when(t == 0)
        def _():
            dst[...] = part

        @pl.when(t > 0)
        def _():
            dst[...] += part

        return 0

    def step(n, _):
        t, q = lax.div(n, 4), lax.rem(n, 4)

        @pl.when((t > 0) & (n < 16) & (j - t >= 0))
        def _():
            z = j - t
            arrive(z, q)

            @pl.when(j < 3)
            def _():
                x_copy(x_held(z, q), z, q, x_up, (j + 1, i)).start()

            x_copy(x_held(z, q), z, q, x_pt, partner).start()

        @pl.when((t > 0) & (n < 16) & (j + t <= 3))
        def _():
            z = j + t
            arrive(z, q)

            @pl.when(j > 0)
            def _():
                x_copy(x_held(z, q), z, q, x_dn, (j - 1, i)).start()

            x_copy(x_held(z, q), z, q, x_pt, partner).start()

        @pl.when(n == 12)
        def _():
            l_pass(xc, 0).wait_recv()
            l_pass(xc, 0).start()

        @pl.when(n == jnp.where(end, 14, 15))
        def _():
            pass_rest()

        @pl.when(n == 14)
        def _():
            sites_first(1)

        lo = jnp.where(n < 14, jnp.maximum(n - 1, 0), n)
        hi = jnp.where(n < 13, n, jnp.where(n < 15, n + 1, n))
        lax.fori_loop(lo, hi, multiply, 0)

        @pl.when(n == 13)
        def _():
            sites_first(0)

        @pl.when(n == 14)
        def _():
            tiles(sites_second)

        return 0

    lax.fori_loop(0, 16, step, 0)

    def finish(n, _):
        half = jnp.where(n == 0, core, 1 - core)
        z = jnp.where(low, 3, 0)
        at_half = pl.ds(pl.multiple_of(half * 128, 128), 128)

        @pl.when(n == 1)
        def _():
            wait_partner(z, 3)

        dst = acc.at[:, :, pl.ds(pl.multiple_of(768 + half * 128, 128), 128)]
        dst[...] += dot_nt(right_part(z), xg[z, 3, at_half, :]).reshape(5, 128, 128)
        sites_last(0, half)
        return 0

    lax.fori_loop(0, 2, finish, 0)

    def left(first, second, t):
        lhs = jnp.concatenate(
            [jnp.concatenate([lg[slot, u] for u in range(5)], axis=1) for slot in (first, second)], axis=0)
        return dot_nt(lhs, vt[t])

    def wait_left(chip_):
        slot = 2 * chip_ + 1 - core
        remote(lg.at[slot], lg.at[slot], l_pt.at[0], l_in.at[slot], partner).wait_recv()

    def send_far(h, t):
        if h == 0:
            return remote(pb.at[0, t], ra.at[t], s_sem.at[0, t], p_sem.at[0, t], at(xc, core))
        return remote(pb.at[1, t], rb.at[t], s_sem.at[1, t], p_sem.at[1, t], at(yc, core))

    def send_x(n, h, t):
        return remote(pb.at[n, t], rx.at[core, t], s_sem.at[n, t], r_sem.at[0, core, t], at(xc, h))

    def send_y(n, h, t):
        return remote(pb.at[n, t], ry.at[core, t], s_sem.at[n, t], r_sem.at[1, core, t], at(yc, h))

    def send_pt(t):
        return remote(pb.at[6, t], rp.at[t], s_sem.at[6, t], p_sem.at[2, t], partner)

    def send_via(h):
        return remote(pb.at[2 + h, 0], rq.at[h], s_sem.at[2 + h, 0], q_in.at[h], (pair, 2 * (yc if h else xc) + core))

    def send_back(h):
        land = ry if h else rx
        return remote(rq.at[h], land.at[core, 0], q_out.at[h], r_sem.at[h, core, 0], (pair, 2 * chip + h))

    def stage(n, _):
        role = jnp.where(n < 4, lax.div(n, 2), jnp.where((n == 4) | (n == 7), 3, 2))
        t = jnp.where(n < 4, lax.rem(n, 2), lax.div(n - 4, 2))

        @pl.when(n == 1)
        def _():
            sites_last(1, 0)
            sites_last(1, 1)

        @pl.when(n == 0)
        def _():
            wait_left(dc)
            wait_left(chip)

        @pl.when(n == 1)
        def _():
            wait_left(xc)
            wait_left(yc)

        def pick(far, near, via, own):
            return jnp.where(role == 0, far, jnp.where(role == 1, near, jnp.where(role == 2, via, own)))

        first = pick(2 * dc, 2 * xc, 2 * yc, 2 * chip + 1 - core)
        second = pick(2 * dc + 1, 2 * yc + 1, 2 * xc + 1, 2 * chip + core)
        res = left(first, second, t)

        @pl.when(role != 2)
        def _():
            pb[2 * role, t] = res[:128]
            pb[2 * role + 1, t] = res[128:]

        @pl.when((n == 7) & jnp.logical_not(end))
        def _():
            for h in range(2):
                send_via(h).wait_recv()
                send_back(h).start()

        @pl.when(role == 2)
        def _():
            send_far(0, t).wait_recv()
            send_far(1, t).wait_recv()
            pb[4, t] = res[:128] + ra[t]
            pb[5, t] = res[128:] + rb[t]
            send_y(4, 0, t).start()
            send_x(5, 1, t).start()

        @pl.when(role == 0)
        def _():
            send_far(0, t).start()
            send_far(1, t).start()

        @pl.when((role == 1) & (end & (t == 0)))
        def _():
            send_via(0).start()
            send_via(1).start()

        @pl.when((role == 1) & jnp.logical_not(end & (t == 0)))
        def _():
            send_x(2, 0, t).start()
            send_y(3, 1, t).start()

        @pl.when(role == 3)
        def _():
            send_pt(t).start()

        return 0

    lax.fori_loop(0, 8, stage, 0)

    def drain(n, _):
        z, q = lax.div(n, 4), lax.rem(n, 4)

        @pl.when((z <= j) & (j < 3))
        def _():
            x_copy(x_held(z, q), z, q, x_up, (j + 1, i)).wait_send()

        @pl.when((z >= j) & (j > 0))
        def _():
            x_copy(x_held(z, q), z, q, x_dn, (j - 1, i)).wait_send()

        x_copy(x_held(z, q), z, q, x_pt, partner).wait_send()
        return 0

    lax.fori_loop(0, 16, drain, 0)
    for n, chip_ in enumerate((xc, yc, dc)):
        l_copy(chip_, n).wait_send()
        l_pass(chip_, n).wait_send()
    l_pass(chip, 3).wait_send()
    for t in range(2):
        send_pt(t).wait_recv()
        for half in range(2):
            remote(rx.at[half, t], rx.at[half, t], s_sem.at[0, t], r_sem.at[0, half, t], partner).wait_recv()
            remote(ry.at[half, t], ry.at[half, t], s_sem.at[0, t], r_sem.at[1, half, t], partner).wait_recv()
        for s in range(2):
            lanes = slice(s * 128, (s + 1) * 128)
            y_ref[pl.ds(s * 4 + core * 2 + t, 128, stride=8), :] = (
                pb[7, t, :, lanes] + (rx[core, t, :, lanes] + ry[core, t, :, lanes]))
            y_ref[pl.ds(s * 4 + (1 - core) * 2 + t, 128, stride=8), :] = (
                rp[t, :, lanes] + (rx[1 - core, t, :, lanes] + ry[1 - core, t, :, lanes]))

    @pl.when(jnp.logical_not(end))
    def _():
        for h in range(2):
            send_back(h).wait_send()

    for t in range(2):
        send_far(0, t).wait_send()
        send_far(1, t).wait_send()
        send_x(2, 0, t).wait_send()
        send_y(3, 1, t).wait_send()
        send_y(4, 0, t).wait_send()
        send_x(5, 1, t).wait_send()
        send_pt(t).wait_send()


def solution(mesh):
    def local_apply(wave, left, mpo, right):
        x = wave.reshape(128, 2, 2, 2, 128).transpose(0, 1, 3, 2, 4).reshape(1024, 128)
        f32, vmem, sem = jnp.float32, pltpu.VMEM, pltpu.SemaphoreType.DMA
        y = pl.pallas_call(
            kernel,
            out_shape=jax.ShapeDtypeStruct((1024, 128), f32),
            in_specs=[pl.BlockSpec(memory_space=pltpu.HBM), pl.BlockSpec(memory_space=pltpu.HBM),
                      pl.BlockSpec(memory_space=pltpu.HBM), pl.BlockSpec(memory_space=pltpu.HBM)],
            out_specs=pl.BlockSpec(memory_space=pltpu.VMEM),
            scratch_shapes=[
                vmem((1024, 128), f32), pltpu.SMEM((5, 2, 2, 5), f32),
                vmem((4, 4, 256, 256), f32), vmem((5, 128, 1024), f32), vmem((5, 128, 1024), f32),
                vmem((2, 5, 128, 256), f32),
                vmem((2, 256, 1280), f32), vmem((8, 5, 128, 256), f32), vmem((8, 2, 128, 256), f32),
                vmem((2, 128, 256), f32), vmem((2, 128, 256), f32), vmem((2, 2, 128, 256), f32),
                vmem((2, 2, 128, 256), f32), vmem((2, 128, 256), f32),
                sem((4, 4)), sem((4, 4)), sem((4, 4)), sem((4, 4, 2)), sem((3,)), sem((4,)), sem((8,)), sem((4,)),
                sem((7, 2)), sem((3, 2)), sem((2, 2, 2)),
                vmem((2, 128, 256), f32), sem((2,)), sem((2,)),
            ],
            compiler_params=pltpu.CompilerParams(collective_id=0, has_side_effects=True,
                                                 vmem_limit_bytes=53 * 1024 * 1024),
        )(x, left.transpose(1, 0, 2), mpo, right.transpose(1, 0, 2))
        return y.reshape(128, 2, 2, 2, 128).transpose(0, 1, 3, 2, 4).reshape(128, 2, 2, 256)

    return jax.shard_map(local_apply, mesh=mesh,
                         in_specs=(P('bx', None, None, 'by'), P('bx', None, None), P(), P('by', None, None)),
                         out_specs=P('bx', None, None, 'by'), check_vma=False)
```

```python
import functools

import jax
import jax.numpy as jnp
from jax import lax
from jax.experimental import pallas as pl
from jax.experimental.pallas import tpu as pltpu
from jax.sharding import PartitionSpec as P

MESH = pl.DeviceIdType.MESH
HIGHEST = lax.Precision.HIGHEST
NT = (((1,), (1,)), ((), ()))


def dot_nt(lhs, rhs):
    return lax.dot_general(lhs, rhs, NT, precision=HIGHEST, preferred_element_type=jnp.float32)


def kernel(x_ref, l_ref, w_hbm, r_ref, y_ref, xv, w_ref, xg, rv, acc, zp, vt, lg, pb, ra, rb, rx, ry, rp,
           x_up, x_dn, x_pt, x_in, l_out, l_pt, l_in, loc, s_sem, p_sem, r_sem, rq, q_out, q_in):
    j, i = lax.axis_index('by'), lax.axis_index('bx')
    chip, core = lax.div(i, 2), lax.rem(i, 2)
    xb, yb = lax.rem(chip, 2), lax.div(chip, 2)
    xc, yc = chip + 1 - 2 * xb, chip + 2 - 4 * yb
    dc = xc + yc - chip
    partner = (j, i + 1 - 2 * core)
    rows = pl.ds(pl.multiple_of(core * 128, 128), 128)
    other_rows = pl.ds(pl.multiple_of((1 - core) * 128, 128), 128)

    def at(chip_, core_):
        return (j, 2 * chip_ + core_)

    def remote(src, dst, send, recv, device):
        return pltpu.make_async_remote_copy(src_ref=src, dst_ref=dst, send_sem=send, recv_sem=recv,
                                            device_id=device, device_id_type=MESH)

    def cols(chip_):
        return pl.ds(pl.multiple_of(chip_ * 256, 256), 256)

    load_r = pltpu.make_async_copy(r_ref.at[:, rows, :], rv, loc.at[0])
    load_x = pltpu.make_async_copy(x_ref, xv, loc.at[1])
    load_w = pltpu.make_async_copy(w_hbm, w_ref, loc.at[3])
    load_l = pltpu.make_async_copy(l_ref.at[:, :, cols(chip)], lg.at[i], loc.at[2])
    load_x.start()
    load_w.start()
    load_r.start()
    load_l.start()

    barrier = pltpu.get_barrier_semaphore()
    end = (j == 0) | (j == 3)
    pair = j + 1 - 2 * lax.rem(j, 2)
    near = [partner, at(xc, 0), at(xc, 1), at(yc, 0), at(yc, 1), at(dc, core),
            (pair, 2 * xc + core), (pair, 2 * yc + core), (pair, 2 * chip + 1 - core)]
    for device in near:
        pl.semaphore_signal(barrier, inc=1, device_id=device, device_id_type=MESH)

    @pl.when(j > 0)
    def _():
        pl.semaphore_signal(barrier, inc=1, device_id=(j - 1, i), device_id_type=MESH)

    @pl.when(j < 3)
    def _():
        pl.semaphore_signal(barrier, inc=1, device_id=(j + 1, i), device_id_type=MESH)

    load_x.wait()
    for p in range(2):
        for half in range(2):
            for q in range(2):
                xg[j, p * 2 + q, rows, half * 128:(half + 1) * 128] = xv[pl.ds(p * 4 + half * 2 + q, 128, stride=8), :]

    @pl.when((j > 0) & (j < 3))
    def _():
        pl.semaphore_wait(barrier, 11)

    @pl.when((j == 0) | (j == 3))
    def _():
        pl.semaphore_wait(barrier, 10)

    def x_copy(src, z, q, sems, device):
        return remote(src, xg.at[z, q, rows, :], sems.at[z, q], x_in.at[z, q, core], device)

    def x_held(z, q):
        return xg.at[z, q, rows, :]

    for q in range(4):
        @pl.when(j < 3)
        def _():
            x_copy(x_held(j, q), j, q, x_up, (j + 1, i)).start()

        @pl.when(j > 0)
        def _():
            x_copy(x_held(j, q), j, q, x_dn, (j - 1, i)).start()

        x_copy(x_held(j, q), j, q, x_pt, partner).start()

    def l_copy(chip_, n):
        return remote(l_ref.at[:, :, cols(chip_)], lg.at[i], l_out.at[n], l_in.at[i], at(chip_, core))

    def l_pass(chip_, n):
        slot = 2 * chip_ + core
        return remote(lg.at[slot], lg.at[slot], l_pt.at[n], l_in.at[slot], partner)

    for n, chip_ in enumerate((xc, yc, dc)):
        l_copy(chip_, n).start()
    load_l.wait()
    l_pass(chip, 3).start()
    load_w.wait()
    load_r.wait()

    def arrive(z, q):
        x_copy(x_held(z, q), z, q, x_pt, partner).wait_recv()

    def wt(u, s, p, v):
        return w_ref[u, s, p, v]

    def field(r, p, q, b):
        return acc[r, b, (p * 2 + q) * 256:(p * 2 + q + 1) * 256]

    def dots(terms):
        total = None
        for weight, value in terms:
            total = value * weight if total is None else total + value * weight
        return total

    def tiles(body):
        def tile(n, _):
            body(pl.ds(pl.multiple_of(n * 16, 16), 16), n * 16)
            return 0

        lax.fori_loop(0, 8, tile, 0)

    def sites_first(t):
        def body(b, start):
            parts = [(q, r, field(r, 0, q, b)) for q in range(2) for r in range(5)]
            mid = [dots((wt(v, t, q, r), x) for q, r, x in parts) for v in range(5)]
            for s in range(2):
                into = pl.ds(pl.multiple_of(s * 128 + start, 16), 16)
                for u in range(5):
                    vt[t, into, u * 256:(u + 1) * 256] = dots((wt(u, s, 0, v), mid[v]) for v in range(5))

        tiles(body)

    def sites_second(b, start):
        parts = [field(r, 1, 0, b) for r in range(5)]
        for t in range(2):
            for v in range(5):
                zp[t, v, b, :] = dots((wt(v, t, 0, r), parts[r]) for r in range(5))

    def sites_last(t, half):
        def tile(n, _):
            b = pl.ds(pl.multiple_of(n * 32, 32), 32)

            def lanes(first):
                return pl.ds(pl.multiple_of(first + half * 128, 128), 128)

            parts = [acc[r, b, lanes(768)] for r in range(5)]
            mid = [zp[t, v, b, lanes(0)] + dots((wt(v, t, 1, r), parts[r]) for r in range(5)) for v in range(5)]
            for s in range(2):
                into = pl.ds(pl.multiple_of(s * 128 + n * 32, 32), 32)
                for u in range(5):
                    vt[t, into, lanes(u * 256)] += dots((wt(u, s, 1, v), mid[v]) for v in range(5))
            return 0

        lax.fori_loop(0, 4, tile, 0)

    low = j < 2
    jm = jnp.where(low, j, 3 - j)

    def pass_rest():
        for n, chip_ in ((2, dc), (1, yc)):
            l_pass(chip_, n).wait_recv()
            l_pass(chip_, n).start()

    def wait_partner(z, q):
        held = xg.at[z, q, other_rows, :]
        remote(held, held, x_pt.at[z, q], x_in.at[z, q, 1 - core], partner).wait_recv()

    def right_part(z):
        return rv[:, :, pl.ds(pl.multiple_of(z * 256, 256), 256)].reshape(640, 256)

    def multiply(m, _):
        t, q = lax.div(m, 4), lax.rem(m, 4)
        zm = jnp.where(t == 0, jm, jnp.where(t == 1, 1 - jm, t))
        z = jnp.where(low, zm, 3 - zm)
        wait_partner(z, q)
        part = dot_nt(right_part(z), xg[z, q]).reshape(5, 128, 256)
        dst = acc.at[:, :, pl.ds(pl.multiple_of(q * 256, 256), 256)]

        @pl.when(t == 0)
        def _():
            dst[...] = part

        @pl.when(t > 0)
        def _():
            dst[...] += part

        return 0

    def ready(n):
        ends = jnp.where(n < 13, n, jnp.minimum(n + 1, 15))
        mids = jnp.where(n < 8, n, jnp.where(n < 11, 2 * n - 7, jnp.minimum(n + 3, 15)))
        return jnp.maximum(jnp.where(end, ends, mids), 0)

    def step(n, _):
        t, q = lax.div(n, 4), lax.rem(n, 4)

        @pl.when((t > 0) & (n < 16) & (j - t >= 0))
        def _():
            z = j - t
            arrive(z, q)

            @pl.when(j < 3)
            def _():
                x_copy(x_held(z, q), z, q, x_up, (j + 1, i)).start()

            x_copy(x_held(z, q), z, q, x_pt, partner).start()

        @pl.when((t > 0) & (n < 16) & (j + t <= 3))
        def _():
            z = j + t
            arrive(z, q)

            @pl.when(j > 0)
            def _():
                x_copy(x_held(z, q), z, q, x_dn, (j - 1, i)).start()

            x_copy(x_held(z, q), z, q, x_pt, partner).start()

        @pl.when(n == 12)
        def _():
            l_pass(xc, 0).wait_recv()
            l_pass(xc, 0).start()

        @pl.when((n == 14) & end)
        def _():
            pass_rest()

        @pl.when(n == 14)
        def _():
            sites_first(1)

        lax.fori_loop(ready(n - 1), ready(n), multiply, 0)

        @pl.when(n == 13)
        def _():
            sites_first(0)

        @pl.when(n == 14)
        def _():
            tiles(sites_second)

        return 0

    lax.fori_loop(0, 16, step, 0)

    def finish(n, _):
        half = jnp.where(n == 0, core, 1 - core)
        z = jnp.where(low, 3, 0)
        at_half = pl.ds(pl.multiple_of(half * 128, 128), 128)

        @pl.when(n == 1)
        def _():
            wait_partner(z, 3)

        dst = acc.at[:, :, pl.ds(pl.multiple_of(768 + half * 128, 128), 128)]
        dst[...] += dot_nt(right_part(z), xg[z, 3, at_half, :]).reshape(5, 128, 128)
        sites_last(0, half)
        return 0

    lax.fori_loop(0, 2, finish, 0)

    @pl.when(jnp.logical_not(end))
    def _():
        pass_rest()


    def left(first, second, t):
        lhs = jnp.concatenate(
            [jnp.concatenate([lg[slot, u] for u in range(5)], axis=1) for slot in (first, second)], axis=0)
        return dot_nt(lhs, vt[t])

    def wait_left(chip_):
        slot = 2 * chip_ + 1 - core
        remote(lg.at[slot], lg.at[slot], l_pt.at[0], l_in.at[slot], partner).wait_recv()

    def send_far(h, t):
        if h == 0:
            return remote(pb.at[0, t], ra.at[t], s_sem.at[0, t], p_sem.at[0, t], at(xc, core))
        return remote(pb.at[1, t], rb.at[t], s_sem.at[1, t], p_sem.at[1, t], at(yc, core))

    def send_x(n, h, t):
        return remote(pb.at[n, t], rx.at[core, t], s_sem.at[n, t], r_sem.at[0, core, t], at(xc, h))

    def send_y(n, h, t):
        return remote(pb.at[n, t], ry.at[core, t], s_sem.at[n, t], r_sem.at[1, core, t], at(yc, h))

    def send_pt(t):
        return remote(pb.at[6, t], rp.at[t], s_sem.at[6, t], p_sem.at[2, t], partner)

    def send_via(h):
        return remote(pb.at[2 + h, 0], rq.at[h], s_sem.at[2 + h, 0], q_in.at[h], (pair, 2 * (yc if h else xc) + core))

    def send_back(h):
        land = ry if h else rx
        return remote(rq.at[h], land.at[core, 0], q_out.at[h], r_sem.at[h, core, 0], (pair, 2 * chip + h))

    def stage(n, _):
        role = jnp.where(n < 4, lax.div(n, 2), jnp.where((n == 4) | (n == 7), 3, 2))
        t = jnp.where(n < 4, lax.rem(n, 2), lax.div(n - 4, 2))

        @pl.when(n == 1)
        def _():
            sites_last(1, 0)
            sites_last(1, 1)

        @pl.when(n == 0)
        def _():
            wait_left(dc)
            wait_left(chip)

        @pl.when(n == 1)
        def _():
            wait_left(xc)
            wait_left(yc)

        def pick(far, near, via, own):
            return jnp.where(role == 0, far, jnp.where(role == 1, near, jnp.where(role == 2, via, own)))

        first = pick(2 * dc, 2 * xc, 2 * yc, 2 * chip + 1 - core)
        second = pick(2 * dc + 1, 2 * yc + 1, 2 * xc + 1, 2 * chip + core)
        res = left(first, second, t)

        @pl.when(role != 2)
        def _():
            pb[2 * role, t] = res[:128]
            pb[2 * role + 1, t] = res[128:]

        @pl.when((n == 7) & jnp.logical_not(end))
        def _():
            for h in range(2):
                send_via(h).wait_recv()
                send_back(h).start()

        @pl.when(role == 2)
        def _():
            send_far(0, t).wait_recv()
            send_far(1, t).wait_recv()
            pb[4, t] = res[:128] + ra[t]
            pb[5, t] = res[128:] + rb[t]
            send_y(4, 0, t).start()
            send_x(5, 1, t).start()

        @pl.when(role == 0)
        def _():
            send_far(0, t).start()
            send_far(1, t).start()

        @pl.when((role == 1) & (end & (t == 0)))
        def _():
            send_via(0).start()
            send_via(1).start()

        @pl.when((role == 1) & jnp.logical_not(end & (t == 0)))
        def _():
            send_x(2, 0, t).start()
            send_y(3, 1, t).start()

        @pl.when(role == 3)
        def _():
            send_pt(t).start()

        return 0

    lax.fori_loop(0, 8, stage, 0)

    def drain(n, _):
        z, q = lax.div(n, 4), lax.rem(n, 4)

        @pl.when((z <= j) & (j < 3))
        def _():
            x_copy(x_held(z, q), z, q, x_up, (j + 1, i)).wait_send()

        @pl.when((z >= j) & (j > 0))
        def _():
            x_copy(x_held(z, q), z, q, x_dn, (j - 1, i)).wait_send()

        x_copy(x_held(z, q), z, q, x_pt, partner).wait_send()
        return 0

    lax.fori_loop(0, 16, drain, 0)
    for n, chip_ in enumerate((xc, yc, dc)):
        l_copy(chip_, n).wait_send()
        l_pass(chip_, n).wait_send()
    l_pass(chip, 3).wait_send()
    for t in range(2):
        send_pt(t).wait_recv()
        for half in range(2):
            remote(rx.at[half, t], rx.at[half, t], s_sem.at[0, t], r_sem.at[0, half, t], partner).wait_recv()
            remote(ry.at[half, t], ry.at[half, t], s_sem.at[0, t], r_sem.at[1, half, t], partner).wait_recv()
        for s in range(2):
            lanes = slice(s * 128, (s + 1) * 128)
            y_ref[pl.ds(s * 4 + core * 2 + t, 128, stride=8), :] = (
                pb[7, t, :, lanes] + (rx[core, t, :, lanes] + ry[core, t, :, lanes]))
            y_ref[pl.ds(s * 4 + (1 - core) * 2 + t, 128, stride=8), :] = (
                rp[t, :, lanes] + (rx[1 - core, t, :, lanes] + ry[1 - core, t, :, lanes]))

    @pl.when(jnp.logical_not(end))
    def _():
        for h in range(2):
            send_back(h).wait_send()

    for t in range(2):
        send_far(0, t).wait_send()
        send_far(1, t).wait_send()
        send_x(2, 0, t).wait_send()
        send_y(3, 1, t).wait_send()
        send_y(4, 0, t).wait_send()
        send_x(5, 1, t).wait_send()
        send_pt(t).wait_send()


def solution(mesh):
    def local_apply(wave, left, mpo, right):
        x = wave.reshape(128, 2, 2, 2, 128).transpose(0, 1, 3, 2, 4).reshape(1024, 128)
        f32, vmem, sem = jnp.float32, pltpu.VMEM, pltpu.SemaphoreType.DMA
        y = pl.pallas_call(
            kernel,
            out_shape=jax.ShapeDtypeStruct((1024, 128), f32),
            in_specs=[pl.BlockSpec(memory_space=pltpu.HBM), pl.BlockSpec(memory_space=pltpu.HBM),
                      pl.BlockSpec(memory_space=pltpu.HBM), pl.BlockSpec(memory_space=pltpu.HBM)],
            out_specs=pl.BlockSpec(memory_space=pltpu.VMEM),
            scratch_shapes=[
                vmem((1024, 128), f32), pltpu.SMEM((5, 2, 2, 5), f32),
                vmem((4, 4, 256, 256), f32), vmem((5, 128, 1024), f32), vmem((5, 128, 1024), f32),
                vmem((2, 5, 128, 256), f32),
                vmem((2, 256, 1280), f32), vmem((8, 5, 128, 256), f32), vmem((8, 2, 128, 256), f32),
                vmem((2, 128, 256), f32), vmem((2, 128, 256), f32), vmem((2, 2, 128, 256), f32),
                vmem((2, 2, 128, 256), f32), vmem((2, 128, 256), f32),
                sem((4, 4)), sem((4, 4)), sem((4, 4)), sem((4, 4, 2)), sem((3,)), sem((4,)), sem((8,)), sem((4,)),
                sem((7, 2)), sem((3, 2)), sem((2, 2, 2)),
                vmem((2, 128, 256), f32), sem((2,)), sem((2,)),
            ],
            compiler_params=pltpu.CompilerParams(collective_id=0, has_side_effects=True,
                                                 vmem_limit_bytes=53 * 1024 * 1024),
        )(x, left.transpose(1, 0, 2), pltpu.with_memory_space_constraint(mpo, pltpu.HBM), right.transpose(1, 0, 2))
        return y.reshape(128, 2, 2, 2, 128).transpose(0, 1, 3, 2, 4).reshape(128, 2, 2, 256)

    return jax.shard_map(local_apply, mesh=mesh,
                         in_specs=(P('bx', None, None, 'by'), P('bx', None, None), P(), P('by', None, None)),
                         out_specs=P('bx', None, None, 'by'), check_vma=False)
```

```python
import functools

import jax
import jax.numpy as jnp
from jax import lax
from jax.experimental import pallas as pl
from jax.experimental.pallas import tpu as pltpu
from jax.sharding import PartitionSpec as P

MESH = pl.DeviceIdType.MESH
HIGHEST = lax.Precision.HIGHEST
NT = (((1,), (1,)), ((), ()))


def dot_nt(lhs, rhs):
    return lax.dot_general(lhs, rhs, NT, precision=HIGHEST, preferred_element_type=jnp.float32)


def kernel(x_ref, l_ref, w_hbm, r_ref, y_ref, xv, w_ref, xg, rv, acc, zp, vt, lg, pb, ra, rb, rx, ry, rp,
           x_up, x_dn, x_pt, x_in, l_out, l_pt, l_in, loc, s_sem, p_sem, r_sem, rq, q_out, q_in):
    j, i = lax.axis_index('by'), lax.axis_index('bx')
    chip, core = lax.div(i, 2), lax.rem(i, 2)
    xb, yb = lax.rem(chip, 2), lax.div(chip, 2)
    xc, yc = chip + 1 - 2 * xb, chip + 2 - 4 * yb
    dc = xc + yc - chip
    partner = (j, i + 1 - 2 * core)
    rows = pl.ds(pl.multiple_of(core * 128, 128), 128)
    other_rows = pl.ds(pl.multiple_of((1 - core) * 128, 128), 128)

    def at(chip_, core_):
        return (j, 2 * chip_ + core_)

    def remote(src, dst, send, recv, device):
        return pltpu.make_async_remote_copy(src_ref=src, dst_ref=dst, send_sem=send, recv_sem=recv,
                                            device_id=device, device_id_type=MESH)

    def cols(chip_):
        return pl.ds(pl.multiple_of(chip_ * 256, 256), 256)

    load_r = pltpu.make_async_copy(r_ref.at[:, rows, :], rv, loc.at[0])
    load_x = pltpu.make_async_copy(x_ref, xv, loc.at[1])
    load_w = pltpu.make_async_copy(w_hbm, w_ref, loc.at[3])
    load_l = pltpu.make_async_copy(l_ref.at[:, :, cols(chip)], lg.at[i], loc.at[2])
    load_x.start()
    load_w.start()
    load_r.start()
    load_l.start()

    barrier = pltpu.get_barrier_semaphore()
    end = (j == 0) | (j == 3)
    pair = j + 1 - 2 * lax.rem(j, 2)
    near = [partner, at(xc, 0), at(xc, 1), at(yc, 0), at(yc, 1), at(dc, core),
            (pair, 2 * xc + core), (pair, 2 * yc + core), (pair, 2 * chip + 1 - core)]
    for device in near:
        pl.semaphore_signal(barrier, inc=1, device_id=device, device_id_type=MESH)

    @pl.when(j > 0)
    def _():
        pl.semaphore_signal(barrier, inc=1, device_id=(j - 1, i), device_id_type=MESH)

    @pl.when(j < 3)
    def _():
        pl.semaphore_signal(barrier, inc=1, device_id=(j + 1, i), device_id_type=MESH)

    load_x.wait()
    for p in range(2):
        for half in range(2):
            for q in range(2):
                xg[j, p * 2 + q, rows, half * 128:(half + 1) * 128] = xv[pl.ds(p * 4 + half * 2 + q, 128, stride=8), :]

    @pl.when((j > 0) & (j < 3))
    def _():
        pl.semaphore_wait(barrier, 11)

    @pl.when((j == 0) | (j == 3))
    def _():
        pl.semaphore_wait(barrier, 10)

    def x_copy(src, z, q, sems, device):
        return remote(src, xg.at[z, q, rows, :], sems, x_in.at[z, q, core], device)

    def x_held(z, q):
        return xg.at[z, q, rows, :]

    for q in range(4):
        @pl.when(j < 3)
        def _():
            x_copy(x_held(j, q), j, q, x_up, (j + 1, i)).start()

        @pl.when(j > 0)
        def _():
            x_copy(x_held(j, q), j, q, x_dn, (j - 1, i)).start()

        x_copy(x_held(j, q), j, q, x_pt, partner).start()

    def l_copy(chip_, n):
        return remote(l_ref.at[:, :, cols(chip_)], lg.at[i], l_out, l_in.at[i], at(chip_, core))

    def l_pass(chip_, n):
        slot = 2 * chip_ + core
        return remote(lg.at[slot], lg.at[slot], l_pt, l_in.at[slot], partner)

    for n, chip_ in enumerate((xc, yc, dc)):
        l_copy(chip_, n).start()
    load_l.wait()
    l_pass(chip, 3).start()
    load_w.wait()
    load_r.wait()

    def arrive(z, q):
        x_copy(x_held(z, q), z, q, x_pt, partner).wait_recv()

    def wt(u, s, p, v):
        return w_ref[u, s, p, v]

    def field(r, p, q, b):
        return acc[r, b, (p * 2 + q) * 256:(p * 2 + q + 1) * 256]

    def dots(terms):
        total = None
        for weight, value in terms:
            total = value * weight if total is None else total + value * weight
        return total

    def tiles(body):
        def tile(n, _):
            body(pl.ds(pl.multiple_of(n * 16, 16), 16), n * 16)
            return 0

        lax.fori_loop(0, 8, tile, 0)

    def sites_first(t):
        def body(b, start):
            parts = [(q, r, field(r, 0, q, b)) for q in range(2) for r in range(5)]
            mid = [dots((wt(v, t, q, r), x) for q, r, x in parts) for v in range(5)]
            for s in range(2):
                into = pl.ds(pl.multiple_of(s * 128 + start, 16), 16)
                for u in range(5):
                    vt[t, into, u * 256:(u + 1) * 256] = dots((wt(u, s, 0, v), mid[v]) for v in range(5))

        tiles(body)

    def sites_second(b, start):
        parts = [field(r, 1, 0, b) for r in range(5)]
        for t in range(2):
            for v in range(5):
                zp[t, v, b, :] = dots((wt(v, t, 0, r), parts[r]) for r in range(5))

    def sites_last(t, half):
        def tile(n, _):
            b = pl.ds(pl.multiple_of(n * 32, 32), 32)

            def lanes(first):
                return pl.ds(pl.multiple_of(first + half * 128, 128), 128)

            parts = [acc[r, b, lanes(768)] for r in range(5)]
            mid = [zp[t, v, b, lanes(0)] + dots((wt(v, t, 1, r), parts[r]) for r in range(5)) for v in range(5)]
            for s in range(2):
                into = pl.ds(pl.multiple_of(s * 128 + n * 32, 32), 32)
                for u in range(5):
                    vt[t, into, lanes(u * 256)] += dots((wt(u, s, 1, v), mid[v]) for v in range(5))
            return 0

        lax.fori_loop(0, 4, tile, 0)

    low = j < 2
    jm = jnp.where(low, j, 3 - j)

    def pass_rest():
        for n, chip_ in ((2, dc), (1, yc)):
            l_pass(chip_, n).wait_recv()
            l_pass(chip_, n).start()

    def wait_partner(z, q):
        held = xg.at[z, q, other_rows, :]
        remote(held, held, x_pt, x_in.at[z, q, 1 - core], partner).wait_recv()

    def right_part(z):
        return rv[:, :, pl.ds(pl.multiple_of(z * 256, 256), 256)].reshape(640, 256)

    def multiply(m, _):
        t, q = lax.div(m, 4), lax.rem(m, 4)
        zm = jnp.where(t == 0, jm, jnp.where(t == 1, 1 - jm, t))
        z = jnp.where(low, zm, 3 - zm)
        wait_partner(z, q)
        part = dot_nt(right_part(z), xg[z, q]).reshape(5, 128, 256)
        dst = acc.at[:, :, pl.ds(pl.multiple_of(q * 256, 256), 256)]

        @pl.when(t == 0)
        def _():
            dst[...] = part

        @pl.when(t > 0)
        def _():
            dst[...] += part

        return 0

    def ready(n):
        ends = jnp.where(n < 13, n, jnp.minimum(n + 1, 15))
        mids = jnp.where(n < 8, n, jnp.where(n < 11, 2 * n - 7, jnp.minimum(n + 3, 15)))
        return jnp.maximum(jnp.where(end, ends, mids), 0)

    def step(n, _):
        t, q = lax.div(n, 4), lax.rem(n, 4)

        @pl.when((t > 0) & (n < 16) & (j - t >= 0))
        def _():
            z = j - t
            arrive(z, q)

            @pl.when(j < 3)
            def _():
                x_copy(x_held(z, q), z, q, x_up, (j + 1, i)).start()

            x_copy(x_held(z, q), z, q, x_pt, partner).start()

        @pl.when((t > 0) & (n < 16) & (j + t <= 3))
        def _():
            z = j + t
            arrive(z, q)

            @pl.when(j > 0)
            def _():
                x_copy(x_held(z, q), z, q, x_dn, (j - 1, i)).start()

            x_copy(x_held(z, q), z, q, x_pt, partner).start()

        @pl.when(n == 12)
        def _():
            l_pass(xc, 0).wait_recv()
            l_pass(xc, 0).start()

        @pl.when((n == 14) & end)
        def _():
            pass_rest()

        @pl.when(n == 14)
        def _():
            sites_first(1)

        lax.fori_loop(ready(n - 1), ready(n), multiply, 0)

        @pl.when(n == 13)
        def _():
            sites_first(0)

        @pl.when(n == 14)
        def _():
            tiles(sites_second)

        return 0

    lax.fori_loop(0, 16, step, 0)

    def finish(n, _):
        half = jnp.where(n == 0, core, 1 - core)
        z = jnp.where(low, 3, 0)
        at_half = pl.ds(pl.multiple_of(half * 128, 128), 128)

        @pl.when(n == 1)
        def _():
            wait_partner(z, 3)

        dst = acc.at[:, :, pl.ds(pl.multiple_of(768 + half * 128, 128), 128)]
        dst[...] += dot_nt(right_part(z), xg[z, 3, at_half, :]).reshape(5, 128, 128)
        sites_last(0, half)
        return 0

    lax.fori_loop(0, 2, finish, 0)

    @pl.when(jnp.logical_not(end))
    def _():
        pass_rest()


    def left(first, second, t):
        lhs = jnp.concatenate(
            [jnp.concatenate([lg[slot, u] for u in range(5)], axis=1) for slot in (first, second)], axis=0)
        return dot_nt(lhs, vt[t])

    def wait_left(chip_):
        slot = 2 * chip_ + 1 - core
        remote(lg.at[slot], lg.at[slot], l_pt, l_in.at[slot], partner).wait_recv()

    def send_far(h, t):
        if h == 0:
            return remote(pb.at[0, t], ra.at[t], s_sem, p_sem.at[0, t], at(xc, core))
        return remote(pb.at[1, t], rb.at[t], s_sem, p_sem.at[1, t], at(yc, core))

    def send_x(n, h, t):
        return remote(pb.at[n, t], rx.at[core, t], s_sem, r_sem.at[0, core, t], at(xc, h))

    def send_y(n, h, t):
        return remote(pb.at[n, t], ry.at[core, t], s_sem, r_sem.at[1, core, t], at(yc, h))

    def send_pt(t):
        return remote(pb.at[6, t], rp.at[t], s_sem, p_sem.at[2, t], partner)

    def send_via(h):
        return remote(pb.at[2 + h, 0], rq.at[h], s_sem, q_in.at[h], (pair, 2 * (yc if h else xc) + core))

    def send_back(h):
        land = ry if h else rx
        return remote(rq.at[h], land.at[core, 0], q_out, r_sem.at[h, core, 0], (pair, 2 * chip + h))

    def stage(n, _):
        role = jnp.where(n < 4, lax.div(n, 2), jnp.where((n == 4) | (n == 7), 3, 2))
        t = jnp.where(n < 4, lax.rem(n, 2), lax.div(n - 4, 2))

        @pl.when(n == 1)
        def _():
            sites_last(1, 0)
            sites_last(1, 1)

        @pl.when(n == 0)
        def _():
            wait_left(dc)
            wait_left(chip)

        @pl.when(n == 1)
        def _():
            wait_left(xc)
            wait_left(yc)

        def pick(far, near, via, own):
            return jnp.where(role == 0, far, jnp.where(role == 1, near, jnp.where(role == 2, via, own)))

        first = pick(2 * dc, 2 * xc, 2 * yc, 2 * chip + 1 - core)
        second = pick(2 * dc + 1, 2 * yc + 1, 2 * xc + 1, 2 * chip + core)
        res = left(first, second, t)

        @pl.when(role != 2)
        def _():
            pb[2 * role, t] = res[:128]
            pb[2 * role + 1, t] = res[128:]

        @pl.when((n == 7) & jnp.logical_not(end))
        def _():
            for h in range(2):
                send_via(h).wait_recv()
                send_back(h).start()

        @pl.when(role == 2)
        def _():
            send_far(0, t).wait_recv()
            send_far(1, t).wait_recv()
            pb[4, t] = res[:128] + ra[t]
            pb[5, t] = res[128:] + rb[t]
            send_y(4, 0, t).start()
            send_x(5, 1, t).start()

        @pl.when(role == 0)
        def _():
            send_far(0, t).start()
            send_far(1, t).start()

        @pl.when((role == 1) & (end & (t == 0)))
        def _():
            send_via(0).start()
            send_via(1).start()

        @pl.when((role == 1) & jnp.logical_not(end & (t == 0)))
        def _():
            send_x(2, 0, t).start()
            send_y(3, 1, t).start()

        @pl.when(role == 3)
        def _():
            send_pt(t).start()

        return 0

    lax.fori_loop(0, 8, stage, 0)

    def sent(what, sem):
        remote(what, what, sem, l_in.at[0], partner).wait_send()

    for blocks in range(1, 4):
        @pl.when(j == blocks - 1)
        def _():
            sent(xg.at[pl.ds(0, blocks), :, rows, :], x_up)

        @pl.when(j == 4 - blocks)
        def _():
            sent(xg.at[pl.ds(0, blocks), :, rows, :], x_dn)

    sent(xg.at[:, :, rows, :], x_pt)
    sent(lg.at[pl.ds(0, 3)], l_out)
    sent(lg.at[pl.ds(0, 4)], l_pt)
    for t in range(2):
        send_pt(t).wait_recv()
        for half in range(2):
            remote(rx.at[half, t], rx.at[half, t], s_sem, r_sem.at[0, half, t], partner).wait_recv()
            remote(ry.at[half, t], ry.at[half, t], s_sem, r_sem.at[1, half, t], partner).wait_recv()
        for s in range(2):
            lanes = slice(s * 128, (s + 1) * 128)
            y_ref[pl.ds(s * 4 + core * 2 + t, 128, stride=8), :] = (
                pb[7, t, :, lanes] + (rx[core, t, :, lanes] + ry[core, t, :, lanes]))
            y_ref[pl.ds(s * 4 + (1 - core) * 2 + t, 128, stride=8), :] = (
                rp[t, :, lanes] + (rx[1 - core, t, :, lanes] + ry[1 - core, t, :, lanes]))

    @pl.when(jnp.logical_not(end))
    def _():
        sent(rq, q_out)

    sent(pb.at[pl.ds(0, 7)], s_sem)


def solution(mesh):
    def local_apply(wave, left, mpo, right):
        x = wave.reshape(128, 2, 2, 2, 128).transpose(0, 1, 3, 2, 4).reshape(1024, 128)
        f32, vmem, sem = jnp.float32, pltpu.VMEM, pltpu.SemaphoreType.DMA
        y = pl.pallas_call(
            kernel,
            out_shape=jax.ShapeDtypeStruct((1024, 128), f32),
            in_specs=[pl.BlockSpec(memory_space=pltpu.HBM), pl.BlockSpec(memory_space=pltpu.HBM),
                      pl.BlockSpec(memory_space=pltpu.HBM), pl.BlockSpec(memory_space=pltpu.HBM)],
            out_specs=pl.BlockSpec(memory_space=pltpu.VMEM),
            scratch_shapes=[
                vmem((1024, 128), f32), pltpu.SMEM((5, 2, 2, 5), f32),
                vmem((4, 4, 256, 256), f32), vmem((5, 128, 1024), f32), vmem((5, 128, 1024), f32),
                vmem((2, 5, 128, 256), f32),
                vmem((2, 256, 1280), f32), vmem((8, 5, 128, 256), f32), vmem((8, 2, 128, 256), f32),
                vmem((2, 128, 256), f32), vmem((2, 128, 256), f32), vmem((2, 2, 128, 256), f32),
                vmem((2, 2, 128, 256), f32), vmem((2, 128, 256), f32),
                sem, sem, sem, sem((4, 4, 2)), sem, sem, sem((8,)), sem((4,)), sem, sem((3, 2)), sem((2, 2, 2)),
                vmem((2, 128, 256), f32), sem, sem((2,)),
            ],
            compiler_params=pltpu.CompilerParams(collective_id=0, has_side_effects=True,
                                                 vmem_limit_bytes=53 * 1024 * 1024),
        )(x, left.transpose(1, 0, 2), pltpu.with_memory_space_constraint(mpo, pltpu.HBM), right.transpose(1, 0, 2))
        return y.reshape(128, 2, 2, 2, 128).transpose(0, 1, 3, 2, 4).reshape(128, 2, 2, 256)

    return jax.shard_map(local_apply, mesh=mesh,
                         in_specs=(P('bx', None, None, 'by'), P('bx', None, None), P(), P('by', None, None)),
                         out_specs=P('bx', None, None, 'by'), check_vma=False)
```

```python
import functools

import jax
import jax.numpy as jnp
from jax import lax
from jax.experimental import pallas as pl
from jax.experimental.pallas import tpu as pltpu
from jax.sharding import PartitionSpec as P

MESH = pl.DeviceIdType.MESH
HIGHEST = lax.Precision.HIGHEST
NT = (((1,), (1,)), ((), ()))


def dot_nt(lhs, rhs):
    return lax.dot_general(lhs, rhs, NT, precision=HIGHEST, preferred_element_type=jnp.float32)


def kernel(x_ref, l_ref, w_hbm, r_ref, y_ref, xv, w_ref, xg, rv, acc, zp, vt, lg, pb, ra, rb, rx, ry, rp,
           x_up, x_dn, x_pt, x_own, x_in, l_out, l_pt, l_in, loc, s_sem, p_sem, r_sem, rq, q_out, q_in):
    j, i = lax.axis_index('by'), lax.axis_index('bx')
    chip, core = lax.div(i, 2), lax.rem(i, 2)
    xb, yb = lax.rem(chip, 2), lax.div(chip, 2)
    xc, yc = chip + 1 - 2 * xb, chip + 2 - 4 * yb
    dc = xc + yc - chip
    partner = (j, i + 1 - 2 * core)
    rows = pl.ds(pl.multiple_of(core * 128, 128), 128)
    other_rows = pl.ds(pl.multiple_of((1 - core) * 128, 128), 128)

    def at(chip_, core_):
        return (j, 2 * chip_ + core_)

    def remote(src, dst, send, recv, device):
        return pltpu.make_async_remote_copy(src_ref=src, dst_ref=dst, send_sem=send, recv_sem=recv,
                                            device_id=device, device_id_type=MESH)

    def cols(chip_):
        return pl.ds(pl.multiple_of(chip_ * 256, 256), 256)

    load_r = pltpu.make_async_copy(r_ref.at[:, rows, :], rv, loc.at[0])
    load_x = pltpu.make_async_copy(x_ref, xv, loc.at[1])
    load_w = pltpu.make_async_copy(w_hbm, w_ref, loc.at[3])
    load_l = pltpu.make_async_copy(l_ref.at[:, :, cols(chip)], lg.at[i], loc.at[2])
    load_x.start()
    load_w.start()
    load_r.start()
    load_l.start()

    barrier = pltpu.get_barrier_semaphore()
    end = (j == 0) | (j == 3)
    pair = j + 1 - 2 * lax.rem(j, 2)
    near = [partner, at(xc, 0), at(xc, 1), at(yc, 0), at(yc, 1), at(dc, core),
            (pair, 2 * xc + core), (pair, 2 * yc + core), (pair, 2 * chip + 1 - core)]
    for device in near:
        pl.semaphore_signal(barrier, inc=1, device_id=device, device_id_type=MESH)

    @pl.when(j > 0)
    def _():
        pl.semaphore_signal(barrier, inc=1, device_id=(j - 1, i), device_id_type=MESH)

    @pl.when(j < 3)
    def _():
        pl.semaphore_signal(barrier, inc=1, device_id=(j + 1, i), device_id_type=MESH)

    load_x.wait()
    for p in range(2):
        for half in range(2):
            for q in range(2):
                xg[j, p * 2 + q, rows, half * 128:(half + 1) * 128] = xv[pl.ds(p * 4 + half * 2 + q, 128, stride=8), :]

    @pl.when((j > 0) & (j < 3))
    def _():
        pl.semaphore_wait(barrier, 11)

    @pl.when((j == 0) | (j == 3))
    def _():
        pl.semaphore_wait(barrier, 10)

    def x_copy(src, z, q, sems, recv, device):
        return remote(src, xg.at[z, q, rows, :], sems, recv, device)

    def up(z, q):
        return x_copy(x_held(z, q), z, q, x_up, x_in.at[z, q, core], (j + 1, i))

    def down(z, q):
        return x_copy(x_held(z, q), z, q, x_dn, x_in.at[z - 1, q, core], (j - 1, i))

    def foreign(z):
        return jnp.where(z > j, z - 1, z)

    def across(z, q):
        return x_copy(x_held(z, q), z, q, x_pt, x_in.at[foreign(z), q, core], partner)

    def x_held(z, q):
        return xg.at[z, q, rows, :]

    for q in range(4):
        @pl.when(j < 3)
        def _():
            up(j, q).start()

        @pl.when(j > 0)
        def _():
            down(j, q).start()

        x_copy(x_held(j, q), j, q, x_pt, x_own, partner).start()

    def l_copy(chip_, n):
        return remote(l_ref.at[:, :, cols(chip_)], lg.at[i], l_out, l_in.at[min(n, 1)], at(chip_, core))

    def l_pass(chip_, n):
        slot = 2 * chip_ + core
        return remote(lg.at[slot], lg.at[slot], l_pt, l_in.at[2 + n // 2], partner)

    def l_wait(count, n):
        held = lg.at[pl.ds(0, count)]
        remote(held, held, l_pt, l_in.at[n], partner).wait_recv()

    for n, chip_ in enumerate((xc, yc, dc)):
        l_copy(chip_, n).start()
    load_l.wait()
    l_pass(chip, 3).start()
    load_w.wait()
    load_r.wait()

    def arrive(z, q):
        x_copy(x_held(z, q), z, q, x_pt, x_in.at[foreign(z), q, core], partner).wait_recv()

    def wt(u, s, p, v):
        return w_ref[u, s, p, v]

    def field(r, p, q, b):
        return acc[r, b, (p * 2 + q) * 256:(p * 2 + q + 1) * 256]

    def dots(terms):
        total = None
        for weight, value in terms:
            total = value * weight if total is None else total + value * weight
        return total

    def tiles(body):
        def tile(n, _):
            body(pl.ds(pl.multiple_of(n * 16, 16), 16), n * 16)
            return 0

        lax.fori_loop(0, 8, tile, 0)

    def sites_first(t):
        def body(b, start):
            parts = [(q, r, field(r, 0, q, b)) for q in range(2) for r in range(5)]
            mid = [dots((wt(v, t, q, r), x) for q, r, x in parts) for v in range(5)]
            for s in range(2):
                into = pl.ds(pl.multiple_of(s * 128 + start, 16), 16)
                for u in range(5):
                    vt[t, into, u * 256:(u + 1) * 256] = dots((wt(u, s, 0, v), mid[v]) for v in range(5))

        tiles(body)

    def sites_second(b, start):
        parts = [field(r, 1, 0, b) for r in range(5)]
        for t in range(2):
            for v in range(5):
                zp[t, v, b, :] = dots((wt(v, t, 0, r), parts[r]) for r in range(5))

    def sites_last(t, half):
        def tile(n, _):
            b = pl.ds(pl.multiple_of(n * 32, 32), 32)

            def lanes(first):
                return pl.ds(pl.multiple_of(first + half * 128, 128), 128)

            parts = [acc[r, b, lanes(768)] for r in range(5)]
            mid = [zp[t, v, b, lanes(0)] + dots((wt(v, t, 1, r), parts[r]) for r in range(5)) for v in range(5)]
            for s in range(2):
                into = pl.ds(pl.multiple_of(s * 128 + n * 32, 32), 32)
                for u in range(5):
                    vt[t, into, lanes(u * 256)] += dots((wt(u, s, 1, v), mid[v]) for v in range(5))
            return 0

        lax.fori_loop(0, 4, tile, 0)

    low = j < 2
    jm = jnp.where(low, j, 3 - j)

    def pass_rest():
        l_wait(2, 1)
        l_pass(dc, 2).start()
        l_pass(yc, 1).start()

    def wait_partner(z, q):
        held = xg.at[z, q, other_rows, :]
        remote(held, held, x_pt, x_in.at[foreign(z), q, 1 - core], partner).wait_recv()

    def right_part(z):
        return rv[:, :, pl.ds(pl.multiple_of(z * 256, 256), 256)].reshape(640, 256)

    def multiply(m, _):
        t, q = lax.div(m, 4), lax.rem(m, 4)
        zm = jnp.where(t == 0, jm, jnp.where(t == 1, 1 - jm, t))
        z = jnp.where(low, zm, 3 - zm)

        @pl.when(m == 0)
        def _():
            held = xg.at[j, :, other_rows, :]
            remote(held, held, x_pt, x_own, partner).wait_recv()

        @pl.when(t > 0)
        def _():
            wait_partner(z, q)

        part = dot_nt(right_part(z), xg[z, q]).reshape(5, 128, 256)
        dst = acc.at[:, :, pl.ds(pl.multiple_of(q * 256, 256), 256)]

        @pl.when(t == 0)
        def _():
            dst[...] = part

        @pl.when(t > 0)
        def _():
            dst[...] += part

        return 0

    def ready(n):
        ends = jnp.where(n < 13, n, jnp.minimum(n + 1, 15))
        mids = jnp.where(n < 8, n, jnp.where(n < 11, 2 * n - 7, jnp.minimum(n + 3, 15)))
        return jnp.maximum(jnp.where(end, ends, mids), 0)

    def step(n, _):
        t, q = lax.div(n, 4), lax.rem(n, 4)

        @pl.when((t > 0) & (n < 16) & (j - t >= 0))
        def _():
            z = j - t
            arrive(z, q)

            @pl.when(j < 3)
            def _():
                up(z, q).start()

            across(z, q).start()

        @pl.when((t > 0) & (n < 16) & (j + t <= 3))
        def _():
            z = j + t
            arrive(z, q)

            @pl.when(j > 0)
            def _():
                down(z, q).start()

            across(z, q).start()

        @pl.when(n == 12)
        def _():
            l_wait(1, 0)
            l_pass(xc, 0).start()

        @pl.when((n == 14) & end)
        def _():
            pass_rest()

        @pl.when(n == 14)
        def _():
            sites_first(1)

        lax.fori_loop(ready(n - 1), ready(n), multiply, 0)

        @pl.when(n == 13)
        def _():
            sites_first(0)

        @pl.when(n == 14)
        def _():
            tiles(sites_second)

        return 0

    lax.fori_loop(0, 16, step, 0)

    def finish(n, _):
        half = jnp.where(n == 0, core, 1 - core)
        z = jnp.where(low, 3, 0)
        at_half = pl.ds(pl.multiple_of(half * 128, 128), 128)

        @pl.when(n == 1)
        def _():
            wait_partner(z, 3)

        dst = acc.at[:, :, pl.ds(pl.multiple_of(768 + half * 128, 128), 128)]
        dst[...] += dot_nt(right_part(z), xg[z, 3, at_half, :]).reshape(5, 128, 128)
        sites_last(0, half)
        return 0

    lax.fori_loop(0, 2, finish, 0)

    @pl.when(jnp.logical_not(end))
    def _():
        pass_rest()


    def left(first, second, t):
        lhs = jnp.concatenate(
            [jnp.concatenate([lg[slot, u] for u in range(5)], axis=1) for slot in (first, second)], axis=0)
        return dot_nt(lhs, vt[t])

    def send_far(h, t):
        if h == 0:
            return remote(pb.at[0, t], ra.at[t], s_sem, p_sem.at[t], at(xc, core))
        return remote(pb.at[1, t], rb.at[t], s_sem, p_sem.at[t], at(yc, core))

    def send_x(n, h, t):
        return remote(pb.at[n, t], rx.at[core, t], s_sem, r_sem.at[t], at(xc, h))

    def send_y(n, h, t):
        return remote(pb.at[n, t], ry.at[core, t], s_sem, r_sem.at[t], at(yc, h))

    def send_pt(t):
        return remote(pb.at[6, t], rp.at[t], s_sem, r_sem.at[t], partner)

    def send_via(h):
        return remote(pb.at[2 + h, 0], rq.at[h], s_sem, q_in.at[h], (pair, 2 * (yc if h else xc) + core))

    def send_back(h):
        land = ry if h else rx
        return remote(rq.at[h], land.at[core, 0], q_out, r_sem.at[0], (pair, 2 * chip + h))

    def stage(n, _):
        role = jnp.where(n < 4, lax.div(n, 2), jnp.where((n == 4) | (n == 7), 3, 2))
        t = jnp.where(n < 4, lax.rem(n, 2), lax.div(n - 4, 2))

        @pl.when(n == 1)
        def _():
            sites_last(1, 0)
            sites_last(1, 1)

        @pl.when(n == 0)
        def _():
            l_wait(2, 3)

        @pl.when(n == 1)
        def _():
            l_wait(2, 2)

        def pick(far, near, via, own):
            return jnp.where(role == 0, far, jnp.where(role == 1, near, jnp.where(role == 2, via, own)))

        first = pick(2 * dc, 2 * xc, 2 * yc, 2 * chip + 1 - core)
        second = pick(2 * dc + 1, 2 * yc + 1, 2 * xc + 1, 2 * chip + core)
        res = left(first, second, t)

        @pl.when(role != 2)
        def _():
            pb[2 * role, t] = res[:128]
            pb[2 * role + 1, t] = res[128:]

        @pl.when((n == 7) & jnp.logical_not(end))
        def _():
            for h in range(2):
                send_via(h).wait_recv()
                send_back(h).start()

        @pl.when(role == 2)
        def _():
            remote(ra, ra, s_sem, p_sem.at[t], partner).wait_recv()
            pb[4, t] = res[:128] + ra[t]
            pb[5, t] = res[128:] + rb[t]
            send_y(4, 0, t).start()
            send_x(5, 1, t).start()

        @pl.when(role == 0)
        def _():
            send_far(0, t).start()
            send_far(1, t).start()

        @pl.when((role == 1) & (end & (t == 0)))
        def _():
            send_via(0).start()
            send_via(1).start()

        @pl.when((role == 1) & jnp.logical_not(end & (t == 0)))
        def _():
            send_x(2, 0, t).start()
            send_y(3, 1, t).start()

        @pl.when(role == 3)
        def _():
            send_pt(t).start()

        return 0

    lax.fori_loop(0, 8, stage, 0)

    def sent(what, sem):
        remote(what, what, sem, l_in.at[0], partner).wait_send()

    for blocks in range(1, 4):
        @pl.when(j == blocks - 1)
        def _():
            sent(xg.at[pl.ds(0, blocks), :, rows, :], x_up)

        @pl.when(j == 4 - blocks)
        def _():
            sent(xg.at[pl.ds(0, blocks), :, rows, :], x_dn)

    sent(xg.at[:, :, rows, :], x_pt)
    sent(lg.at[pl.ds(0, 3)], l_out)
    sent(lg.at[pl.ds(0, 4)], l_pt)
    for t in range(2):
        five = pb.at[pl.ds(0, 5), t]
        remote(five, five, s_sem, r_sem.at[t], partner).wait_recv()
        for s in range(2):
            lanes = slice(s * 128, (s + 1) * 128)
            y_ref[pl.ds(s * 4 + core * 2 + t, 128, stride=8), :] = (
                pb[7, t, :, lanes] + (rx[core, t, :, lanes] + ry[core, t, :, lanes]))
            y_ref[pl.ds(s * 4 + (1 - core) * 2 + t, 128, stride=8), :] = (
                rp[t, :, lanes] + (rx[1 - core, t, :, lanes] + ry[1 - core, t, :, lanes]))

    @pl.when(jnp.logical_not(end))
    def _():
        sent(rq, q_out)

    sent(pb.at[pl.ds(0, 7)], s_sem)


def solution(mesh):
    def local_apply(wave, left, mpo, right):
        x = wave.reshape(128, 2, 2, 2, 128).transpose(0, 1, 3, 2, 4).reshape(1024, 128)
        f32, vmem, sem = jnp.float32, pltpu.VMEM, pltpu.SemaphoreType.DMA
        y = pl.pallas_call(
            kernel,
            out_shape=jax.ShapeDtypeStruct((1024, 128), f32),
            in_specs=[pl.BlockSpec(memory_space=pltpu.HBM), pl.BlockSpec(memory_space=pltpu.HBM),
                      pl.BlockSpec(memory_space=pltpu.HBM), pl.BlockSpec(memory_space=pltpu.HBM)],
            out_specs=pl.BlockSpec(memory_space=pltpu.VMEM),
            scratch_shapes=[
                vmem((1024, 128), f32), pltpu.SMEM((5, 2, 2, 5), f32),
                vmem((4, 4, 256, 256), f32), vmem((5, 128, 1024), f32), vmem((5, 128, 1024), f32),
                vmem((2, 5, 128, 256), f32),
                vmem((2, 256, 1280), f32), vmem((8, 5, 128, 256), f32), vmem((8, 2, 128, 256), f32),
                vmem((2, 128, 256), f32), vmem((2, 128, 256), f32), vmem((2, 2, 128, 256), f32),
                vmem((2, 2, 128, 256), f32), vmem((2, 128, 256), f32),
                sem, sem, sem, sem, sem((3, 4, 2)), sem, sem, sem((4,)), sem((4,)), sem, sem((2,)), sem((2,)),
                vmem((2, 128, 256), f32), sem, sem((2,)),
            ],
            compiler_params=pltpu.CompilerParams(collective_id=0, has_side_effects=True,
                                                 vmem_limit_bytes=53 * 1024 * 1024),
        )(x, left.transpose(1, 0, 2), pltpu.with_memory_space_constraint(mpo, pltpu.HBM), right.transpose(1, 0, 2))
        return y.reshape(128, 2, 2, 2, 128).transpose(0, 1, 3, 2, 4).reshape(128, 2, 2, 256)

    return jax.shard_map(local_apply, mesh=mesh,
                         in_specs=(P('bx', None, None, 'by'), P('bx', None, None), P(), P('by', None, None)),
                         out_specs=P('bx', None, None, 'by'), check_vma=False)
```

```python
import functools

import jax
import jax.numpy as jnp
from jax import lax
from jax.experimental import pallas as pl
from jax.experimental.pallas import tpu as pltpu
from jax.sharding import PartitionSpec as P

MESH = pl.DeviceIdType.MESH
HIGHEST = lax.Precision.HIGHEST
NT = (((1,), (1,)), ((), ()))


def dot_nt(lhs, rhs):
    return lax.dot_general(lhs, rhs, NT, precision=HIGHEST, preferred_element_type=jnp.float32)


def kernel(x_ref, l_ref, w_hbm, r_ref, y_ref, xv, w_ref, xg, rv, acc, zp, vt, lg, pb, ra, rb, rx, ry, rp,
           x_up, x_dn, x_pt, x_own, x_in, l_out, l_pt, l_in, loc, s_sem, p_sem, r_sem, rq, q_out, q_in, here):
    j, i = lax.axis_index('by'), lax.axis_index('bx')
    chip, core = lax.div(i, 2), lax.rem(i, 2)
    xb, yb = lax.rem(chip, 2), lax.div(chip, 2)
    xc, yc = chip + 1 - 2 * xb, chip + 2 - 4 * yb
    dc = xc + yc - chip
    partner = (j, i + 1 - 2 * core)
    rows = pl.ds(pl.multiple_of(core * 128, 128), 128)
    other_rows = pl.ds(pl.multiple_of((1 - core) * 128, 128), 128)

    def at(chip_, core_):
        return (j, 2 * chip_ + core_)

    def remote(src, dst, send, recv, device):
        return pltpu.make_async_remote_copy(src_ref=src, dst_ref=dst, send_sem=send, recv_sem=recv,
                                            device_id=device, device_id_type=MESH)

    def cols(chip_):
        return pl.ds(pl.multiple_of(chip_ * 256, 256), 256)

    load_r = pltpu.make_async_copy(r_ref.at[:, rows, :], rv, loc.at[0])
    load_x = pltpu.make_async_copy(x_ref, xv, loc.at[1])
    load_w = pltpu.make_async_copy(w_hbm, w_ref, loc.at[3])
    load_l = pltpu.make_async_copy(l_ref.at[:, :, cols(chip)], lg.at[i], loc.at[2])
    load_x.start()

    end = (j == 0) | (j == 3)
    odd = lax.rem(j, 2)
    pair = j + 1 - 2 * odd
    below, above = lax.div(j + 2, 3), 1 - lax.div(j, 3)

    groups = [
        (core, [partner]),
        (xb, [at(xc, 0), at(xc, 1)]),
        (yb, [at(yc, 0), at(yc, 1), at(dc, core)]),
        (odd, [(pair, 2 * xc + core), (pair, 2 * yc + core), (pair, 2 * chip + 1 - core)]),
    ]
    barrier = pltpu.get_barrier_semaphore()

    @pl.when(j < 3)
    def _():
        pl.semaphore_signal(barrier, inc=1, device_id=(j + 1, i), device_id_type=MESH)

    for last, peers in groups:
        @pl.when(last == 0)
        def _():
            for device in peers:
                pl.semaphore_signal(barrier, inc=1, device_id=device, device_id_type=MESH)

    load_w.start()
    load_r.start()
    load_l.start()
    ahead = core + 2 * xb + 3 * yb + 3 * odd + below
    @pl.when(ahead > 0)
    def _():
        pl.semaphore_wait(barrier, ahead)

    @pl.when(j > 0)
    def _():
        pl.semaphore_signal(here, inc=1, device_id=(j - 1, i), device_id_type=MESH)

    for last, peers in groups:
        @pl.when(last == 1)
        def _():
            for device in peers:
                pl.semaphore_signal(here, inc=1, device_id=device, device_id_type=MESH)

    load_x.wait()
    for p in range(2):
        for half in range(2):
            for q in range(2):
                xg[j, p * 2 + q, rows, half * 128:(half + 1) * 128] = xv[pl.ds(p * 4 + half * 2 + q, 128, stride=8), :]

    def x_copy(src, z, q, sems, recv, device):
        return remote(src, xg.at[z, q, rows, :], sems, recv, device)

    def up(z, q):
        return x_copy(x_held(z, q), z, q, x_up, x_in.at[z, q, core], (j + 1, i))

    def down(z, q):
        return x_copy(x_held(z, q), z, q, x_dn, x_in.at[z - 1, q, core], (j - 1, i))

    def foreign(z):
        return jnp.where(z > j, z - 1, z)

    def across(z, q):
        return x_copy(x_held(z, q), z, q, x_pt, x_in.at[foreign(z), q, core], partner)

    def x_held(z, q):
        return xg.at[z, q, rows, :]

    @pl.when(j > 0)
    def _():
        for q in range(4):
            down(j, q).start()

    behind = (1 - core) + 2 * (1 - xb) + 3 * (1 - yb) + 3 * (1 - odd) + above

    @pl.when(behind > 0)
    def _():
        pl.semaphore_wait(here, behind)

    for q in range(4):
        @pl.when(j < 3)
        def _():
            up(j, q).start()

        x_copy(x_held(j, q), j, q, x_pt, x_own, partner).start()

    def l_copy(chip_, n):
        return remote(l_ref.at[:, :, cols(chip_)], lg.at[i], l_out, l_in.at[min(n, 1)], at(chip_, core))

    def l_pass(chip_, n):
        slot = 2 * chip_ + core
        return remote(lg.at[slot], lg.at[slot], l_pt, l_in.at[2 + n // 2], partner)

    def l_wait(count, n):
        held = lg.at[pl.ds(0, count)]
        remote(held, held, l_pt, l_in.at[n], partner).wait_recv()

    for n, chip_ in enumerate((xc, yc, dc)):
        l_copy(chip_, n).start()
    load_l.wait()
    l_pass(chip, 3).start()
    load_w.wait()
    load_r.wait()

    def arrive(z, q):
        x_copy(x_held(z, q), z, q, x_pt, x_in.at[foreign(z), q, core], partner).wait_recv()

    def wt(u, s, p, v):
        return w_ref[u, s, p, v]

    def field(r, p, q, b):
        return acc[r, b, (p * 2 + q) * 256:(p * 2 + q + 1) * 256]

    def dots(terms):
        total = None
        for weight, value in terms:
            total = value * weight if total is None else total + value * weight
        return total

    def tiles(body):
        def tile(n, _):
            body(pl.ds(pl.multiple_of(n * 16, 16), 16), n * 16)
            return 0

        lax.fori_loop(0, 8, tile, 0, unroll=2)

    def sites_first(t):
        def body(b, start):
            parts = [(q, r, field(r, 0, q, b)) for q in range(2) for r in range(5)]
            mid = [dots((wt(v, t, q, r), x) for q, r, x in parts) for v in range(5)]
            for s in range(2):
                into = pl.ds(pl.multiple_of(s * 128 + start, 16), 16)
                for u in range(5):
                    vt[t, into, u * 256:(u + 1) * 256] = dots((wt(u, s, 0, v), mid[v]) for v in range(5))

        tiles(body)

    def sites_second(b, start):
        parts = [field(r, 1, 0, b) for r in range(5)]
        for t in range(2):
            for v in range(5):
                zp[t, v, b, :] = dots((wt(v, t, 0, r), parts[r]) for r in range(5))

    def sites_last(t, half):
        def tile(n, _):
            b = pl.ds(pl.multiple_of(n * 32, 32), 32)

            def lanes(first):
                return pl.ds(pl.multiple_of(first + half * 128, 128), 128)

            parts = [acc[r, b, lanes(768)] for r in range(5)]
            mid = [zp[t, v, b, lanes(0)] + dots((wt(v, t, 1, r), parts[r]) for r in range(5)) for v in range(5)]
            for s in range(2):
                into = pl.ds(pl.multiple_of(s * 128 + n * 32, 32), 32)
                for u in range(5):
                    vt[t, into, lanes(u * 256)] += dots((wt(u, s, 1, v), mid[v]) for v in range(5))
            return 0

        lax.fori_loop(0, 4, tile, 0, unroll=True)

    low = j < 2
    jm = jnp.where(low, j, 3 - j)

    def pass_rest():
        l_wait(2, 1)
        l_pass(dc, 2).start()
        l_pass(yc, 1).start()

    def wait_partner(z, q):
        held = xg.at[z, q, other_rows, :]
        remote(held, held, x_pt, x_in.at[foreign(z), q, 1 - core], partner).wait_recv()

    def right_part(z):
        return rv[:, :, pl.ds(pl.multiple_of(z * 256, 256), 256)].reshape(640, 256)

    def multiply(m, _):
        t, q = lax.div(m, 4), lax.rem(m, 4)
        zm = jnp.where(t == 0, jm, jnp.where(t == 1, 1 - jm, t))
        z = jnp.where(low, zm, 3 - zm)

        @pl.when(m == 0)
        def _():
            held = xg.at[j, :, other_rows, :]
            remote(held, held, x_pt, x_own, partner).wait_recv()

        @pl.when(t > 0)
        def _():
            wait_partner(z, q)

        part = dot_nt(right_part(z), xg[z, q]).reshape(5, 128, 256)
        dst = acc.at[:, :, pl.ds(pl.multiple_of(q * 256, 256), 256)]

        @pl.when(t == 0)
        def _():
            dst[...] = part

        @pl.when(t > 0)
        def _():
            dst[...] += part

        return 0

    def ready(n):
        ends = jnp.where(n < 13, n, jnp.minimum(n + 1, 15))
        mids = jnp.where(n < 8, n, jnp.where(n < 11, 2 * n - 7, jnp.minimum(n + 3, 15)))
        return jnp.maximum(jnp.where(end, ends, mids), 0)

    def step(n, _):
        t, q = lax.div(n, 4), lax.rem(n, 4)

        @pl.when((t > 0) & (n < 16) & (j - t >= 0))
        def _():
            z = j - t
            arrive(z, q)

            @pl.when(j < 3)
            def _():
                up(z, q).start()

            across(z, q).start()

        @pl.when((t > 0) & (n < 16) & (j + t <= 3))
        def _():
            z = j + t
            arrive(z, q)

            @pl.when(j > 0)
            def _():
                down(z, q).start()

            across(z, q).start()

        @pl.when(n == 12)
        def _():
            l_wait(1, 0)
            l_pass(xc, 0).start()

        @pl.when((n == 14) & end)
        def _():
            pass_rest()

        @pl.when(n == 14)
        def _():
            sites_first(1)

        lax.fori_loop(ready(n - 1), ready(n), multiply, 0)

        @pl.when(n == 13)
        def _():
            sites_first(0)

        @pl.when(n == 14)
        def _():
            tiles(sites_second)

        return 0

    lax.fori_loop(0, 16, step, 0)

    def finish(n, _):
        half = jnp.where(n == 0, core, 1 - core)
        z = jnp.where(low, 3, 0)
        at_half = pl.ds(pl.multiple_of(half * 128, 128), 128)

        @pl.when(n == 1)
        def _():
            wait_partner(z, 3)

        dst = acc.at[:, :, pl.ds(pl.multiple_of(768 + half * 128, 128), 128)]
        dst[...] += dot_nt(right_part(z), xg[z, 3, at_half, :]).reshape(5, 128, 128)
        sites_last(0, half)
        return 0

    lax.fori_loop(0, 2, finish, 0)

    @pl.when(jnp.logical_not(end))
    def _():
        pass_rest()


    def left(first, second, t):
        lhs = jnp.concatenate(
            [jnp.concatenate([lg[slot, u] for u in range(5)], axis=1) for slot in (first, second)], axis=0)
        return dot_nt(lhs, vt[t])

    def send_far(h, t):
        if h == 0:
            return remote(pb.at[0, t], ra.at[t], s_sem, p_sem.at[t], at(xc, core))
        return remote(pb.at[1, t], rb.at[t], s_sem, p_sem.at[t], at(yc, core))

    def send_x(n, h, t):
        return remote(pb.at[n, t], rx.at[core, t], s_sem, r_sem.at[t], at(xc, h))

    def send_y(n, h, t):
        return remote(pb.at[n, t], ry.at[core, t], s_sem, r_sem.at[t], at(yc, h))

    def send_pt(t):
        return remote(pb.at[6, t], rp.at[t], s_sem, r_sem.at[t], partner)

    def send_via(h):
        return remote(pb.at[2 + h, 0], rq.at[h], s_sem, q_in.at[h], (pair, 2 * (yc if h else xc) + core))

    def send_back(h):
        land = ry if h else rx
        return remote(rq.at[h], land.at[core, 0], q_out, r_sem.at[0], (pair, 2 * chip + h))

    def stage(n, _):
        role = jnp.where(n < 4, lax.div(n, 2), jnp.where((n == 4) | (n == 7), 3, 2))
        t = jnp.where(n < 4, lax.rem(n, 2), lax.div(n - 4, 2))

        @pl.when(n == 1)
        def _():
            sites_last(1, 0)
            sites_last(1, 1)

        @pl.when(n == 0)
        def _():
            l_wait(2, 3)

        @pl.when(n == 1)
        def _():
            l_wait(2, 2)

        def pick(far, near, via, own):
            return jnp.where(role == 0, far, jnp.where(role == 1, near, jnp.where(role == 2, via, own)))

        first = pick(2 * dc, 2 * xc, 2 * yc, 2 * chip + 1 - core)
        second = pick(2 * dc + 1, 2 * yc + 1, 2 * xc + 1, 2 * chip + core)
        res = left(first, second, t)

        @pl.when(role != 2)
        def _():
            pb[2 * role, t] = res[:128]
            pb[2 * role + 1, t] = res[128:]

        @pl.when((n == 7) & jnp.logical_not(end))
        def _():
            for h in range(2):
                send_via(h).wait_recv()
                send_back(h).start()

        @pl.when(role == 2)
        def _():
            remote(ra, ra, s_sem, p_sem.at[t], partner).wait_recv()
            pb[4, t] = res[:128] + ra[t]
            pb[5, t] = res[128:] + rb[t]
            send_y(4, 0, t).start()
            send_x(5, 1, t).start()

        @pl.when(role == 0)
        def _():
            send_far(0, t).start()
            send_far(1, t).start()

        @pl.when((role == 1) & (end & (t == 0)))
        def _():
            send_via(0).start()
            send_via(1).start()

        @pl.when((role == 1) & jnp.logical_not(end & (t == 0)))
        def _():
            send_x(2, 0, t).start()
            send_y(3, 1, t).start()

        @pl.when(role == 3)
        def _():
            send_pt(t).start()

        return 0

    lax.fori_loop(0, 8, stage, 0)

    def sent(what, sem):
        remote(what, what, sem, l_in.at[0], partner).wait_send()

    for blocks in range(1, 4):
        @pl.when(j == blocks - 1)
        def _():
            sent(xg.at[pl.ds(0, blocks), :, rows, :], x_up)

        @pl.when(j == 4 - blocks)
        def _():
            sent(xg.at[pl.ds(0, blocks), :, rows, :], x_dn)

    sent(xg.at[:, :, rows, :], x_pt)
    sent(lg.at[pl.ds(0, 3)], l_out)
    sent(lg.at[pl.ds(0, 4)], l_pt)
    for t in range(2):
        five = pb.at[pl.ds(0, 5), t]
        remote(five, five, s_sem, r_sem.at[t], partner).wait_recv()
        for s in range(2):
            lanes = slice(s * 128, (s + 1) * 128)
            y_ref[pl.ds(s * 4 + core * 2 + t, 128, stride=8), :] = (
                pb[7, t, :, lanes] + (rx[core, t, :, lanes] + ry[core, t, :, lanes]))
            y_ref[pl.ds(s * 4 + (1 - core) * 2 + t, 128, stride=8), :] = (
                rp[t, :, lanes] + (rx[1 - core, t, :, lanes] + ry[1 - core, t, :, lanes]))

    @pl.when(jnp.logical_not(end))
    def _():
        sent(rq, q_out)

    sent(pb.at[pl.ds(0, 7)], s_sem)


def solution(mesh):
    def local_apply(wave, left, mpo, right):
        x = wave.reshape(128, 2, 2, 2, 128).transpose(0, 1, 3, 2, 4).reshape(1024, 128)
        f32, vmem, sem = jnp.float32, pltpu.VMEM, pltpu.SemaphoreType.DMA
        y = pl.pallas_call(
            kernel,
            out_shape=jax.ShapeDtypeStruct((1024, 128), f32),
            in_specs=[pl.BlockSpec(memory_space=pltpu.HBM), pl.BlockSpec(memory_space=pltpu.HBM),
                      pl.BlockSpec(memory_space=pltpu.HBM), pl.BlockSpec(memory_space=pltpu.HBM)],
            out_specs=pl.BlockSpec(memory_space=pltpu.VMEM),
            scratch_shapes=[
                vmem((1024, 128), f32), pltpu.SMEM((5, 2, 2, 5), f32),
                vmem((4, 4, 256, 256), f32), vmem((5, 128, 1024), f32), vmem((5, 128, 1024), f32),
                vmem((2, 5, 128, 256), f32),
                vmem((2, 256, 1280), f32), vmem((8, 5, 128, 256), f32), vmem((8, 2, 128, 256), f32),
                vmem((2, 128, 256), f32), vmem((2, 128, 256), f32), vmem((2, 2, 128, 256), f32),
                vmem((2, 2, 128, 256), f32), vmem((2, 128, 256), f32),
                sem, sem, sem, sem, sem((3, 4, 2)), sem, sem, sem((4,)), sem((4,)), sem, sem((2,)), sem((2,)),
                vmem((2, 128, 256), f32), sem, sem((2,)), pltpu.SemaphoreType.REGULAR,
            ],
            compiler_params=pltpu.CompilerParams(collective_id=0, has_side_effects=True,
                                                 vmem_limit_bytes=53 * 1024 * 1024),
        )(x, left.transpose(1, 0, 2), pltpu.with_memory_space_constraint(mpo, pltpu.HBM), right.transpose(1, 0, 2))
        return y.reshape(128, 2, 2, 2, 128).transpose(0, 1, 3, 2, 4).reshape(128, 2, 2, 256)

    return jax.shard_map(local_apply, mesh=mesh,
                         in_specs=(P('bx', None, None, 'by'), P('bx', None, None), P(), P('by', None, None)),
                         out_specs=P('bx', None, None, 'by'), check_vma=False)
```

```python
import functools

import jax
import jax.numpy as jnp
from jax import lax
from jax.experimental import pallas as pl
from jax.experimental.pallas import tpu as pltpu
from jax.sharding import PartitionSpec as P

MESH = pl.DeviceIdType.MESH
HIGHEST = lax.Precision.HIGHEST
NT = (((1,), (1,)), ((), ()))


def dot_nt(lhs, rhs):
    return lax.dot_general(lhs, rhs, NT, precision=HIGHEST, preferred_element_type=jnp.float32)


def kernel(x_ref, l_ref, w_hbm, r_ref, y_ref, xv, w_ref, xg, rv, acc, zp, vt, lg, pb, ra, rb, rx, ry, rp,
           x_up, x_pt, x_own, x_in, l_pt, l_in, loc, s_sem, p_sem, r_sem, rq, q_in, here):
    j, i = lax.axis_index('by'), lax.axis_index('bx')
    chip, core = lax.div(i, 2), lax.rem(i, 2)
    xb, yb = lax.rem(chip, 2), lax.div(chip, 2)
    xc, yc = chip + 1 - 2 * xb, chip + 2 - 4 * yb
    dc = xc + yc - chip
    partner = (j, i + 1 - 2 * core)
    rows = pl.ds(pl.multiple_of(core * 128, 128), 128)
    other_rows = pl.ds(pl.multiple_of((1 - core) * 128, 128), 128)

    def at(chip_, core_):
        return (j, 2 * chip_ + core_)

    def remote(src, dst, send, recv, device):
        return pltpu.make_async_remote_copy(src_ref=src, dst_ref=dst, send_sem=send, recv_sem=recv,
                                            device_id=device, device_id_type=MESH)

    def cols(chip_):
        return pl.ds(pl.multiple_of(chip_ * 256, 256), 256)

    load_r = pltpu.make_async_copy(r_ref.at[:, rows, :], rv, loc.at[0])
    load_x = pltpu.make_async_copy(x_ref, xv, loc.at[1])
    load_w = pltpu.make_async_copy(w_hbm, w_ref, loc.at[3])
    load_l = pltpu.make_async_copy(l_ref.at[:, :, cols(chip)], lg.at[i], loc.at[2])
    load_x.start()

    end = (j == 0) | (j == 3)
    odd = lax.rem(j, 2)
    pair = j + 1 - 2 * odd
    below, above = lax.div(j + 2, 3), 1 - lax.div(j, 3)

    groups = [
        (core, [partner]),
        (xb, [at(xc, 0), at(xc, 1)]),
        (yb, [at(yc, 0), at(yc, 1), at(dc, core)]),
        (odd, [(pair, 2 * xc + core), (pair, 2 * yc + core), (pair, 2 * chip + 1 - core)]),
    ]
    barrier = pltpu.get_barrier_semaphore()

    @pl.when(j < 3)
    def _():
        pl.semaphore_signal(barrier, inc=1, device_id=(j + 1, i), device_id_type=MESH)

    for last, peers in groups:
        @pl.when(last == 0)
        def _():
            for device in peers:
                pl.semaphore_signal(barrier, inc=1, device_id=device, device_id_type=MESH)

    load_w.start()
    load_r.start()
    load_l.start()
    ahead = core + 2 * xb + 3 * yb + 3 * odd + below
    @pl.when(ahead > 0)
    def _():
        pl.semaphore_wait(barrier, ahead)

    @pl.when(j > 0)
    def _():
        pl.semaphore_signal(here, inc=1, device_id=(j - 1, i), device_id_type=MESH)

    for last, peers in groups:
        @pl.when(last == 1)
        def _():
            for device in peers:
                pl.semaphore_signal(here, inc=1, device_id=device, device_id_type=MESH)

    load_x.wait()
    for p in range(2):
        for half in range(2):
            for q in range(2):
                xg[j, p * 2 + q, rows, half * 128:(half + 1) * 128] = xv[pl.ds(p * 4 + half * 2 + q, 128, stride=8), :]

    def x_copy(src, z, q, sems, recv, device):
        return remote(src, xg.at[z, q, rows, :], sems, recv, device)

    def up(z, q):
        return x_copy(x_held(z, q), z, q, x_up, x_in.at[z, q, core], (j + 1, i))

    def down(z, q):
        return x_copy(x_held(z, q), z, q, x_up, x_in.at[z - 1, q, core], (j - 1, i))

    def foreign(z):
        return jnp.where(z > j, z - 1, z)

    def across(z, q):
        return x_copy(x_held(z, q), z, q, x_pt, x_in.at[foreign(z), q, core], partner)

    def x_held(z, q):
        return xg.at[z, q, rows, :]

    @pl.when(j > 0)
    def _():
        for q in range(4):
            down(j, q).start()

    behind = (1 - core) + 2 * (1 - xb) + 3 * (1 - yb) + 3 * (1 - odd) + above

    @pl.when(behind > 0)
    def _():
        pl.semaphore_wait(here, behind)

    for q in range(4):
        @pl.when(j < 3)
        def _():
            up(j, q).start()

        x_copy(x_held(j, q), j, q, x_pt, x_own, partner).start()

    def l_copy(chip_, n):
        return remote(l_ref.at[:, :, cols(chip_)], lg.at[i], l_pt, l_in.at[min(n, 1)], at(chip_, core))

    def l_pass(chip_, n):
        slot = 2 * chip_ + core
        return remote(lg.at[slot], lg.at[slot], l_pt, l_in.at[2 + n // 2], partner)

    def l_wait(count, n):
        held = lg.at[pl.ds(0, count)]
        remote(held, held, l_pt, l_in.at[n], partner).wait_recv()

    for n, chip_ in enumerate((xc, yc, dc)):
        l_copy(chip_, n).start()
    load_l.wait()
    l_pass(chip, 3).start()
    load_w.wait()
    load_r.wait()

    def arrive(z, q):
        x_copy(x_held(z, q), z, q, x_pt, x_in.at[foreign(z), q, core], partner).wait_recv()

    def wt(u, s, p, v):
        return w_ref[u, s, p, v]

    def field(r, p, q, b):
        return acc[r, b, (p * 2 + q) * 256:(p * 2 + q + 1) * 256]

    def dots(terms):
        total = None
        for weight, value in terms:
            total = value * weight if total is None else total + value * weight
        return total

    def tiles(body):
        def tile(n, _):
            body(pl.ds(pl.multiple_of(n * 16, 16), 16), n * 16)
            return 0

        lax.fori_loop(0, 8, tile, 0, unroll=2)

    def sites_first(t):
        def body(b, start):
            parts = [(q, r, field(r, 0, q, b)) for q in range(2) for r in range(5)]
            mid = [dots((wt(v, t, q, r), x) for q, r, x in parts) for v in range(5)]
            for s in range(2):
                into = pl.ds(pl.multiple_of(s * 128 + start, 16), 16)
                for u in range(5):
                    vt[t, into, u * 256:(u + 1) * 256] = dots((wt(u, s, 0, v), mid[v]) for v in range(5))

        tiles(body)

    def sites_second(b, start):
        parts = [field(r, 1, 0, b) for r in range(5)]
        for t in range(2):
            for v in range(5):
                zp[t, v, b, :] = dots((wt(v, t, 0, r), parts[r]) for r in range(5))

    def sites_last(t, half):
        def tile(n, _):
            b = pl.ds(pl.multiple_of(n * 32, 32), 32)

            def lanes(first):
                return pl.ds(pl.multiple_of(first + half * 128, 128), 128)

            parts = [acc[r, b, lanes(768)] for r in range(5)]
            mid = [zp[t, v, b, lanes(0)] + dots((wt(v, t, 1, r), parts[r]) for r in range(5)) for v in range(5)]
            for s in range(2):
                into = pl.ds(pl.multiple_of(s * 128 + n * 32, 32), 32)
                for u in range(5):
                    vt[t, into, lanes(u * 256)] += dots((wt(u, s, 1, v), mid[v]) for v in range(5))
            return 0

        lax.fori_loop(0, 4, tile, 0, unroll=True)

    low = j < 2
    jm = jnp.where(low, j, 3 - j)

    def pass_rest():
        l_wait(2, 1)
        l_pass(dc, 2).start()
        l_pass(yc, 1).start()

    def wait_partner(z, q):
        held = xg.at[z, q, other_rows, :]
        remote(held, held, x_pt, x_in.at[foreign(z), q, 1 - core], partner).wait_recv()

    def right_part(z):
        return rv[:, :, pl.ds(pl.multiple_of(z * 256, 256), 256)].reshape(640, 256)

    def multiply(m, _):
        t, q = lax.div(m, 4), lax.rem(m, 4)
        zm = jnp.where(t == 0, jm, jnp.where(t == 1, 1 - jm, t))
        z = jnp.where(low, zm, 3 - zm)

        @pl.when(m == 0)
        def _():
            held = xg.at[j, :, other_rows, :]
            remote(held, held, x_pt, x_own, partner).wait_recv()

        @pl.when(t > 0)
        def _():
            wait_partner(z, q)

        part = dot_nt(right_part(z), xg[z, q]).reshape(5, 128, 256)
        dst = acc.at[:, :, pl.ds(pl.multiple_of(q * 256, 256), 256)]

        @pl.when(t == 0)
        def _():
            dst[...] = part

        @pl.when(t > 0)
        def _():
            dst[...] += part

        return 0

    def ready(n):
        ends = jnp.where(n < 13, n, jnp.minimum(n + 1, 15))
        mids = jnp.where(n < 8, n, jnp.where(n < 11, 2 * n - 7, jnp.minimum(n + 3, 15)))
        return jnp.maximum(jnp.where(end, ends, mids), 0)

    def step(n, _):
        t, q = lax.div(n, 4), lax.rem(n, 4)

        @pl.when((t > 0) & (n < 16) & (j - t >= 0))
        def _():
            z = j - t
            arrive(z, q)

            @pl.when(j < 3)
            def _():
                up(z, q).start()

            across(z, q).start()

        @pl.when((t > 0) & (n < 16) & (j + t <= 3))
        def _():
            z = j + t
            arrive(z, q)

            @pl.when(j > 0)
            def _():
                down(z, q).start()

            across(z, q).start()

        @pl.when(n == 12)
        def _():
            l_wait(1, 0)
            l_pass(xc, 0).start()

        @pl.when((n == 14) & end)
        def _():
            pass_rest()

        @pl.when(n == 14)
        def _():
            sites_first(1)

        lax.fori_loop(ready(n - 1), ready(n), multiply, 0)

        @pl.when(n == 13)
        def _():
            sites_first(0)

        @pl.when(n == 14)
        def _():
            tiles(sites_second)

        return 0

    lax.fori_loop(0, 16, step, 0)

    def finish(n, _):
        half = jnp.where(n == 0, core, 1 - core)
        z = jnp.where(low, 3, 0)
        at_half = pl.ds(pl.multiple_of(half * 128, 128), 128)

        @pl.when(n == 1)
        def _():
            wait_partner(z, 3)

        dst = acc.at[:, :, pl.ds(pl.multiple_of(768 + half * 128, 128), 128)]
        dst[...] += dot_nt(right_part(z), xg[z, 3, at_half, :]).reshape(5, 128, 128)
        sites_last(0, half)
        return 0

    lax.fori_loop(0, 2, finish, 0)

    @pl.when(jnp.logical_not(end))
    def _():
        pass_rest()


    def left(first, second, t):
        lhs = jnp.concatenate(
            [jnp.concatenate([lg[slot, u] for u in range(5)], axis=1) for slot in (first, second)], axis=0)
        return dot_nt(lhs, vt[t])

    def send_far(h, t):
        if h == 0:
            return remote(pb.at[0, t], ra.at[t], s_sem, p_sem.at[t], at(xc, core))
        return remote(pb.at[1, t], rb.at[t], s_sem, p_sem.at[t], at(yc, core))

    def send_x(n, h, t):
        return remote(pb.at[n, t], rx.at[core, t], s_sem, r_sem.at[t], at(xc, h))

    def send_y(n, h, t):
        return remote(pb.at[n, t], ry.at[core, t], s_sem, r_sem.at[t], at(yc, h))

    def send_pt(t):
        return remote(pb.at[6, t], rp.at[t], s_sem, r_sem.at[t], partner)

    def send_via(h):
        return remote(pb.at[2 + h, 0], rq.at[h], s_sem, q_in.at[h], (pair, 2 * (yc if h else xc) + core))

    def send_back(h):
        land = ry if h else rx
        return remote(rq.at[h], land.at[core, 0], s_sem, r_sem.at[0], (pair, 2 * chip + h))

    def stage(n, _):
        role = jnp.where(n < 4, lax.div(n, 2), jnp.where((n == 4) | (n == 7), 3, 2))
        t = jnp.where(n < 4, lax.rem(n, 2), lax.div(n - 4, 2))

        @pl.when(n == 1)
        def _():
            sites_last(1, 0)
            sites_last(1, 1)

        @pl.when(n == 0)
        def _():
            l_wait(2, 3)

        @pl.when(n == 1)
        def _():
            l_wait(2, 2)

        def pick(far, near, via, own):
            return jnp.where(role == 0, far, jnp.where(role == 1, near, jnp.where(role == 2, via, own)))

        first = pick(2 * dc, 2 * xc, 2 * yc, 2 * chip + 1 - core)
        second = pick(2 * dc + 1, 2 * yc + 1, 2 * xc + 1, 2 * chip + core)
        res = left(first, second, t)

        @pl.when(role != 2)
        def _():
            pb[2 * role, t] = res[:128]
            pb[2 * role + 1, t] = res[128:]

        @pl.when((n == 7) & jnp.logical_not(end))
        def _():
            for h in range(2):
                send_via(h).wait_recv()
                send_back(h).start()

        @pl.when(role == 2)
        def _():
            remote(ra, ra, s_sem, p_sem.at[t], partner).wait_recv()
            pb[4, t] = res[:128] + ra[t]
            pb[5, t] = res[128:] + rb[t]
            send_y(4, 0, t).start()
            send_x(5, 1, t).start()

        @pl.when(role == 0)
        def _():
            send_far(0, t).start()
            send_far(1, t).start()

        @pl.when((role == 1) & (end & (t == 0)))
        def _():
            send_via(0).start()
            send_via(1).start()

        @pl.when((role == 1) & jnp.logical_not(end & (t == 0)))
        def _():
            send_x(2, 0, t).start()
            send_y(3, 1, t).start()

        @pl.when(role == 3)
        def _():
            send_pt(t).start()

        return 0

    lax.fori_loop(0, 8, stage, 0)

    def sent(what, sem):
        remote(what, what, sem, l_in.at[0], partner).wait_send()

    @pl.when(end)
    def _():
        sent(xg.at[0, :, rows, :], x_up)

    @pl.when(jnp.logical_not(end))
    def _():
        sent(lg.at[pl.ds(0, 4)], x_up)

    sent(xg.at[:, :, rows, :], x_pt)
    sent(lg.at[pl.ds(0, 7)], l_pt)
    for t in range(2):
        five = pb.at[pl.ds(0, 5), t]
        remote(five, five, s_sem, r_sem.at[t], partner).wait_recv()
        for s in range(2):
            lanes = slice(s * 128, (s + 1) * 128)
            y_ref[pl.ds(s * 4 + core * 2 + t, 128, stride=8), :] = (
                pb[7, t, :, lanes] + (rx[core, t, :, lanes] + ry[core, t, :, lanes]))
            y_ref[pl.ds(s * 4 + (1 - core) * 2 + t, 128, stride=8), :] = (
                rp[t, :, lanes] + (rx[1 - core, t, :, lanes] + ry[1 - core, t, :, lanes]))

    @pl.when(jnp.logical_not(end))
    def _():
        sent(pb, s_sem)

    @pl.when(end)
    def _():
        sent(pb.at[pl.ds(0, 7)], s_sem)


def solution(mesh):
    def local_apply(wave, left, mpo, right):
        x = wave.reshape(128, 2, 2, 2, 128).transpose(0, 1, 3, 2, 4).reshape(1024, 128)
        f32, vmem, sem = jnp.float32, pltpu.VMEM, pltpu.SemaphoreType.DMA
        y = pl.pallas_call(
            kernel,
            out_shape=jax.ShapeDtypeStruct((1024, 128), f32),
            in_specs=[pl.BlockSpec(memory_space=pltpu.HBM), pl.BlockSpec(memory_space=pltpu.HBM),
                      pl.BlockSpec(memory_space=pltpu.HBM), pl.BlockSpec(memory_space=pltpu.HBM)],
            out_specs=pl.BlockSpec(memory_space=pltpu.VMEM),
            scratch_shapes=[
                vmem((1024, 128), f32), pltpu.SMEM((5, 2, 2, 5), f32),
                vmem((4, 4, 256, 256), f32), vmem((5, 128, 1024), f32), vmem((5, 128, 1024), f32),
                vmem((2, 5, 128, 256), f32),
                vmem((2, 256, 1280), f32), vmem((8, 5, 128, 256), f32), vmem((8, 2, 128, 256), f32),
                vmem((2, 128, 256), f32), vmem((2, 128, 256), f32), vmem((2, 2, 128, 256), f32),
                vmem((2, 2, 128, 256), f32), vmem((2, 128, 256), f32),
                sem, sem, sem, sem((3, 4, 2)), sem, sem((4,)), sem((4,)), sem, sem((2,)), sem((2,)),
                vmem((2, 128, 256), f32), sem((2,)), pltpu.SemaphoreType.REGULAR,
            ],
            compiler_params=pltpu.CompilerParams(collective_id=0, has_side_effects=True,
                                                 vmem_limit_bytes=53 * 1024 * 1024),
        )(x, left.transpose(1, 0, 2), pltpu.with_memory_space_constraint(mpo, pltpu.HBM), right.transpose(1, 0, 2))
        return y.reshape(128, 2, 2, 2, 128).transpose(0, 1, 3, 2, 4).reshape(128, 2, 2, 256)

    return jax.shard_map(local_apply, mesh=mesh,
                         in_specs=(P('bx', None, None, 'by'), P('bx', None, None), P(), P('by', None, None)),
                         out_specs=P('bx', None, None, 'by'), check_vma=False)
```

```python
import functools

import jax
import jax.numpy as jnp
from jax import lax
from jax.experimental import pallas as pl
from jax.experimental.pallas import tpu as pltpu
from jax.sharding import PartitionSpec as P

MESH = pl.DeviceIdType.MESH
HIGHEST = lax.Precision.HIGHEST
NT = (((1,), (1,)), ((), ()))


def dot_nt(lhs, rhs):
    return lax.dot_general(lhs, rhs, NT, precision=HIGHEST, preferred_element_type=jnp.float32)


def kernel(x_ref, l_ref, w_hbm, r_ref, y_ref, xv, w_ref, xg, rv, acc, zp, vt, lg, pb, ra, rb, rx, ry, rp,
           x_up, x_pt, x_own, x_in, l_pt, l_in, loc, s_sem, p_sem, r_sem, rq, q_in, here):
    j, i = lax.axis_index('by'), lax.axis_index('bx')
    chip, core = lax.div(i, 2), lax.rem(i, 2)
    xb, yb = lax.rem(chip, 2), lax.div(chip, 2)
    xc, yc = chip + 1 - 2 * xb, chip + 2 - 4 * yb
    dc = xc + yc - chip
    partner = (j, i + 1 - 2 * core)
    rows = pl.ds(pl.multiple_of(core * 128, 128), 128)
    other_rows = pl.ds(pl.multiple_of((1 - core) * 128, 128), 128)

    def at(chip_, core_):
        return (j, 2 * chip_ + core_)

    def remote(src, dst, send, recv, device):
        return pltpu.make_async_remote_copy(src_ref=src, dst_ref=dst, send_sem=send, recv_sem=recv,
                                            device_id=device, device_id_type=MESH)

    def cols(chip_):
        return pl.ds(pl.multiple_of(chip_ * 256, 256), 256)

    load_r = pltpu.make_async_copy(r_ref.at[:, rows, :], rv, loc.at[0])
    load_x = pltpu.make_async_copy(x_ref, xv, loc.at[1])
    load_w = pltpu.make_async_copy(w_hbm, w_ref, loc.at[2])
    load_l = pltpu.make_async_copy(l_ref.at[:, :, cols(chip)], lg.at[i], loc.at[0])
    load_x.start()

    end = (j == 0) | (j == 3)
    odd = lax.rem(j, 2)
    pair = j + 1 - 2 * odd
    below, above = lax.div(j + 2, 3), 1 - lax.div(j, 3)

    groups = [
        (core, [partner]),
        (xb, [at(xc, 0), at(xc, 1)]),
        (yb, [at(yc, 0), at(yc, 1), at(dc, core)]),
        (odd, [(pair, 2 * xc + core), (pair, 2 * yc + core), (pair, 2 * chip + 1 - core)]),
    ]
    barrier = pltpu.get_barrier_semaphore()

    @pl.when(j < 3)
    def _():
        pl.semaphore_signal(barrier, inc=1, device_id=(j + 1, i), device_id_type=MESH)

    for last, peers in groups:
        @pl.when(last == 0)
        def _():
            for device in peers:
                pl.semaphore_signal(barrier, inc=1, device_id=device, device_id_type=MESH)

    load_w.start()
    load_r.start()
    load_l.start()
    ahead = core + 2 * xb + 3 * yb + 3 * odd + below
    @pl.when(ahead > 0)
    def _():
        pl.semaphore_wait(barrier, ahead)

    @pl.when(j > 0)
    def _():
        pl.semaphore_signal(here, inc=1, device_id=(j - 1, i), device_id_type=MESH)

    for last, peers in groups:
        @pl.when(last == 1)
        def _():
            for device in peers:
                pl.semaphore_signal(here, inc=1, device_id=device, device_id_type=MESH)

    load_x.wait()
    for p in range(2):
        for half in range(2):
            for q in range(2):
                xg[j, p * 2 + q, rows, half * 128:(half + 1) * 128] = xv[pl.ds(p * 4 + half * 2 + q, 128, stride=8), :]

    def x_copy(src, z, q, sems, recv, device):
        return remote(src, xg.at[z, q, rows, :], sems, recv, device)

    def up(z, q):
        return x_copy(x_held(z, q), z, q, x_up, x_in.at[z, q, core], (j + 1, i))

    def down(z, q):
        return x_copy(x_held(z, q), z, q, x_up, x_in.at[z - 1, q, core], (j - 1, i))

    def foreign(z):
        return jnp.where(z > j, z - 1, z)

    def across(z, q):
        return x_copy(x_held(z, q), z, q, x_pt, x_in.at[foreign(z), q, core], partner)

    def x_held(z, q):
        return xg.at[z, q, rows, :]

    @pl.when(j > 0)
    def _():
        for q in range(4):
            down(j, q).start()

    behind = (1 - core) + 2 * (1 - xb) + 3 * (1 - yb) + 3 * (1 - odd) + above

    @pl.when(behind > 0)
    def _():
        pl.semaphore_wait(here, behind)

    for q in range(4):
        @pl.when(j < 3)
        def _():
            up(j, q).start()

        x_copy(x_held(j, q), j, q, x_pt, x_own, partner).start()

    def l_copy(chip_, n):
        return remote(l_ref.at[:, :, cols(chip_)], lg.at[i], l_pt, l_in.at[min(n, 1)], at(chip_, core))

    def l_pass(chip_, n):
        slot = 2 * chip_ + core
        return remote(lg.at[slot], lg.at[slot], l_pt, l_in.at[2 + n // 2], partner)

    def l_wait(count, n):
        held = lg.at[pl.ds(0, count)]
        remote(held, held, l_pt, l_in.at[n], partner).wait_recv()

    for n, chip_ in enumerate((xc, yc, dc)):
        l_copy(chip_, n).start()
    both = lg.at[pl.ds(0, 5)]
    pltpu.make_async_copy(both, both, loc.at[0]).wait()
    l_pass(chip, 3).start()
    load_w.wait()

    def arrive(z, q):
        x_copy(x_held(z, q), z, q, x_pt, x_in.at[foreign(z), q, core], partner).wait_recv()

    def wt(u, s, p, v):
        return w_ref[u, s, p, v]

    def field(r, p, q, b):
        return acc[r, b, (p * 2 + q) * 256:(p * 2 + q + 1) * 256]

    def dots(terms):
        total = None
        for weight, value in terms:
            total = value * weight if total is None else total + value * weight
        return total

    def tiles(body):
        def tile(n, _):
            body(pl.ds(pl.multiple_of(n * 16, 16), 16), n * 16)
            return 0

        lax.fori_loop(0, 8, tile, 0, unroll=2)

    def sites_first(t):
        def body(b, start):
            parts = [(q, r, field(r, 0, q, b)) for q in range(2) for r in range(5)]
            mid = [dots((wt(v, t, q, r), x) for q, r, x in parts) for v in range(5)]
            for s in range(2):
                into = pl.ds(pl.multiple_of(s * 128 + start, 16), 16)
                for u in range(5):
                    vt[t, into, u * 256:(u + 1) * 256] = dots((wt(u, s, 0, v), mid[v]) for v in range(5))

        tiles(body)

    def sites_second(b, start):
        parts = [field(r, 1, 0, b) for r in range(5)]
        for t in range(2):
            for v in range(5):
                zp[t, v, b, :] = dots((wt(v, t, 0, r), parts[r]) for r in range(5))

    def sites_last(t, half):
        def tile(n, _):
            b = pl.ds(pl.multiple_of(n * 32, 32), 32)

            def lanes(first):
                return pl.ds(pl.multiple_of(first + half * 128, 128), 128)

            parts = [acc[r, b, lanes(768)] for r in range(5)]
            mid = [zp[t, v, b, lanes(0)] + dots((wt(v, t, 1, r), parts[r]) for r in range(5)) for v in range(5)]
            for s in range(2):
                into = pl.ds(pl.multiple_of(s * 128 + n * 32, 32), 32)
                for u in range(5):
                    vt[t, into, lanes(u * 256)] += dots((wt(u, s, 1, v), mid[v]) for v in range(5))
            return 0

        lax.fori_loop(0, 4, tile, 0, unroll=True)

    low = j < 2
    jm = jnp.where(low, j, 3 - j)

    def pass_rest():
        l_wait(2, 1)
        l_pass(dc, 2).start()
        l_pass(yc, 1).start()

    def wait_partner(z, q):
        held = xg.at[z, q, other_rows, :]
        remote(held, held, x_pt, x_in.at[foreign(z), q, 1 - core], partner).wait_recv()

    def right_part(z):
        return rv[:, :, pl.ds(pl.multiple_of(z * 256, 256), 256)].reshape(640, 256)

    def multiply(m, _):
        t, q = lax.div(m, 4), lax.rem(m, 4)
        zm = jnp.where(t == 0, jm, jnp.where(t == 1, 1 - jm, t))
        z = jnp.where(low, zm, 3 - zm)

        @pl.when(m == 0)
        def _():
            held = xg.at[j, :, other_rows, :]
            remote(held, held, x_pt, x_own, partner).wait_recv()

        @pl.when(t > 0)
        def _():
            wait_partner(z, q)

        part = dot_nt(right_part(z), xg[z, q]).reshape(5, 128, 256)
        dst = acc.at[:, :, pl.ds(pl.multiple_of(q * 256, 256), 256)]

        @pl.when(t == 0)
        def _():
            dst[...] = part

        @pl.when(t > 0)
        def _():
            dst[...] += part

        return 0

    def ready(n):
        ends = jnp.where(n < 13, n, jnp.minimum(n + 1, 15))
        mids = jnp.where(n < 8, n, jnp.where(n < 11, 2 * n - 7, jnp.minimum(n + 3, 15)))
        return jnp.maximum(jnp.where(end, ends, mids), 0)

    def step(n, _):
        t, q = lax.div(n, 4), lax.rem(n, 4)

        @pl.when((t > 0) & (n < 16) & (j - t >= 0))
        def _():
            z = j - t
            arrive(z, q)

            @pl.when(j < 3)
            def _():
                up(z, q).start()

            across(z, q).start()

        @pl.when((t > 0) & (n < 16) & (j + t <= 3))
        def _():
            z = j + t
            arrive(z, q)

            @pl.when(j > 0)
            def _():
                down(z, q).start()

            across(z, q).start()

        @pl.when(n == 12)
        def _():
            l_wait(1, 0)
            l_pass(xc, 0).start()

        @pl.when((n == 14) & end)
        def _():
            pass_rest()

        @pl.when(n == 14)
        def _():
            sites_first(1)

        lax.fori_loop(ready(n - 1), ready(n), multiply, 0)

        @pl.when(n == 13)
        def _():
            sites_first(0)

        @pl.when(n == 14)
        def _():
            tiles(sites_second)

        return 0

    lax.fori_loop(0, 16, step, 0)

    def finish(n, _):
        half = jnp.where(n == 0, core, 1 - core)
        z = jnp.where(low, 3, 0)
        at_half = pl.ds(pl.multiple_of(half * 128, 128), 128)

        @pl.when(n == 1)
        def _():
            wait_partner(z, 3)

        dst = acc.at[:, :, pl.ds(pl.multiple_of(768 + half * 128, 128), 128)]
        dst[...] += dot_nt(right_part(z), xg[z, 3, at_half, :]).reshape(5, 128, 128)
        sites_last(0, half)
        return 0

    lax.fori_loop(0, 2, finish, 0)

    @pl.when(jnp.logical_not(end))
    def _():
        pass_rest()


    def left(first, second, t):
        lhs = jnp.concatenate(
            [jnp.concatenate([lg[slot, u] for u in range(5)], axis=1) for slot in (first, second)], axis=0)
        return dot_nt(lhs, vt[t])

    def send_far(h, t):
        if h == 0:
            return remote(pb.at[0, t], ra.at[t], s_sem, p_sem.at[t], at(xc, core))
        return remote(pb.at[1, t], rb.at[t], s_sem, p_sem.at[t], at(yc, core))

    def send_x(n, h, t):
        return remote(pb.at[n, t], rx.at[core, t], s_sem, r_sem.at[t], at(xc, h))

    def send_y(n, h, t):
        return remote(pb.at[n, t], ry.at[core, t], s_sem, r_sem.at[t], at(yc, h))

    def send_pt(t):
        return remote(pb.at[6, t], rp.at[t], s_sem, r_sem.at[t], partner)

    def send_via(h):
        return remote(pb.at[2 + h, 0], rq.at[h], s_sem, q_in.at[h], (pair, 2 * (yc if h else xc) + core))

    def send_back(h):
        land = ry if h else rx
        return remote(rq.at[h], land.at[core, 0], s_sem, r_sem.at[0], (pair, 2 * chip + h))

    def stage(n, _):
        role = jnp.where(n < 4, lax.div(n, 2), jnp.where((n == 4) | (n == 7), 3, 2))
        t = jnp.where(n < 4, lax.rem(n, 2), lax.div(n - 4, 2))

        @pl.when(n == 1)
        def _():
            sites_last(1, 0)
            sites_last(1, 1)

        @pl.when(n == 0)
        def _():
            l_wait(2, 3)

        @pl.when(n == 1)
        def _():
            l_wait(2, 2)

        def pick(far, near, via, own):
            return jnp.where(role == 0, far, jnp.where(role == 1, near, jnp.where(role == 2, via, own)))

        first = pick(2 * dc, 2 * xc, 2 * yc, 2 * chip + 1 - core)
        second = pick(2 * dc + 1, 2 * yc + 1, 2 * xc + 1, 2 * chip + core)
        res = left(first, second, t)

        @pl.when(role != 2)
        def _():
            pb[2 * role, t] = res[:128]
            pb[2 * role + 1, t] = res[128:]

        @pl.when((n == 7) & jnp.logical_not(end))
        def _():
            for h in range(2):
                send_via(h).wait_recv()
                send_back(h).start()

        @pl.when(role == 2)
        def _():
            remote(ra, ra, s_sem, p_sem.at[t], partner).wait_recv()
            pb[4, t] = res[:128] + ra[t]
            pb[5, t] = res[128:] + rb[t]
            send_y(4, 0, t).start()
            send_x(5, 1, t).start()

        @pl.when(role == 0)
        def _():
            send_far(0, t).start()
            send_far(1, t).start()

        @pl.when((role == 1) & (end & (t == 0)))
        def _():
            send_via(0).start()
            send_via(1).start()

        @pl.when((role == 1) & jnp.logical_not(end & (t == 0)))
        def _():
            send_x(2, 0, t).start()
            send_y(3, 1, t).start()

        @pl.when(role == 3)
        def _():
            send_pt(t).start()

        return 0

    lax.fori_loop(0, 8, stage, 0)

    def sent(what, sem):
        remote(what, what, sem, l_in.at[0], partner).wait_send()

    @pl.when(end)
    def _():
        sent(xg.at[0, :, rows, :], x_up)

    @pl.when(jnp.logical_not(end))
    def _():
        sent(lg.at[pl.ds(0, 4)], x_up)

    sent(xg.at[:, :, rows, :], x_pt)
    sent(lg.at[pl.ds(0, 7)], l_pt)
    for t in range(2):
        five = pb.at[pl.ds(0, 5), t]
        remote(five, five, s_sem, r_sem.at[t], partner).wait_recv()
        for s in range(2):
            lanes = slice(s * 128, (s + 1) * 128)
            y_ref[pl.ds(s * 4 + core * 2 + t, 128, stride=8), :] = (
                pb[7, t, :, lanes] + (rx[core, t, :, lanes] + ry[core, t, :, lanes]))
            y_ref[pl.ds(s * 4 + (1 - core) * 2 + t, 128, stride=8), :] = (
                rp[t, :, lanes] + (rx[1 - core, t, :, lanes] + ry[1 - core, t, :, lanes]))

    @pl.when(jnp.logical_not(end))
    def _():
        sent(pb, s_sem)

    @pl.when(end)
    def _():
        sent(pb.at[pl.ds(0, 7)], s_sem)


def solution(mesh):
    def local_apply(wave, left, mpo, right):
        x = wave.reshape(128, 2, 2, 2, 128).transpose(0, 1, 3, 2, 4).reshape(1024, 128)
        f32, vmem, sem = jnp.float32, pltpu.VMEM, pltpu.SemaphoreType.DMA
        y = pl.pallas_call(
            kernel,
            out_shape=jax.ShapeDtypeStruct((1024, 128), f32),
            in_specs=[pl.BlockSpec(memory_space=pltpu.HBM), pl.BlockSpec(memory_space=pltpu.HBM),
                      pl.BlockSpec(memory_space=pltpu.HBM), pl.BlockSpec(memory_space=pltpu.HBM)],
            out_specs=pl.BlockSpec(memory_space=pltpu.VMEM),
            scratch_shapes=[
                vmem((1024, 128), f32), pltpu.SMEM((5, 2, 2, 5), f32),
                vmem((4, 4, 256, 256), f32), vmem((5, 128, 1024), f32), vmem((5, 128, 1024), f32),
                vmem((2, 5, 128, 256), f32),
                vmem((2, 256, 1280), f32), vmem((8, 5, 128, 256), f32), vmem((8, 2, 128, 256), f32),
                vmem((2, 128, 256), f32), vmem((2, 128, 256), f32), vmem((2, 2, 128, 256), f32),
                vmem((2, 2, 128, 256), f32), vmem((2, 128, 256), f32),
                sem, sem, sem, sem((3, 4, 2)), sem, sem((4,)), sem((3,)), sem, sem((2,)), sem((2,)),
                vmem((2, 128, 256), f32), sem((2,)), pltpu.SemaphoreType.REGULAR,
            ],
            compiler_params=pltpu.CompilerParams(collective_id=0, has_side_effects=True,
                                                 vmem_limit_bytes=53 * 1024 * 1024),
        )(x, left.transpose(1, 0, 2), pltpu.with_memory_space_constraint(mpo, pltpu.HBM), right.transpose(1, 0, 2))
        return y.reshape(128, 2, 2, 2, 128).transpose(0, 1, 3, 2, 4).reshape(128, 2, 2, 256)

    return jax.shard_map(local_apply, mesh=mesh,
                         in_specs=(P('bx', None, None, 'by'), P('bx', None, None), P(), P('by', None, None)),
                         out_specs=P('bx', None, None, 'by'), check_vma=False)
```
